32 devices in a mesh: cfg: 2 (over y), space: 8 (over z, x), tm: 2 (over core).
Axes of the slice: x: 2, y: 2, z: 4, core: 2. Of those that a mesh axis runs over, the one named last changes fastest.
Arguments:
- eigvecs: bfloat16 [4, 2304, 3, 2, 128], P(('cfg', 'tm'), 'space'), parts along dimension 0, may hold values from -6 to 6
- perambulator: bfloat16 [4, 8, 4, 2, 128, 128], P(('cfg', 'tm'), None, None, None, 'space'), parts along dimension 0, may hold values from -1 to 4
- momenta: int32 [1, 3], replicated, may hold values from 1 to 3
- source_slots: int32 [2], replicated, may hold values from 0 to 7, as said below
- gamma_columns: int32 [12, 4], replicated, may hold values from 0 to 3, each once within a row
- gamma_phases: int32 [12, 4], replicated, may hold values from 0 to 3
Outputs:
- meson: float32 [4, 128, 1, 12, 2, 128], P(('cfg', 'tm'), 'space'), parts along dimension 0
The draws below stay inside these ranges and needn't reach their ends.
There are 2 independent parts, one for each index of `cfg`. The reference program is written for one: setup_inputs(seed, part) draws one part's arguments, and reference() takes and returns one part's arrays. A program takes and returns all parts, laid end to end along the dimension named above; an argument that names none is the same for every part. Nothing has to cross between parts.
Inputs may be any that keep to these rules, and one draw needn't show every extreme that they name: `source_slots`: the two slots differ, and one of them is 7. `gamma_columns`: each row is a permutation of 0 to 3.
All inputs are finite; a program needn't handle non-finite values.
Results may differ from the reference program's by a relative error of at most 0.0049.
Values may be sent and summed in bfloat16 or wider, within the bound.
A program may use at most 64 MiB of HBM per device.

```python
import math
import jax
import jax.numpy as jnp
from jax import lax

NEV = 128
NSTORE = 8
NMOM = 1
NGAM = 12
LY = 48
LZ = 48
NT = 2
SITES = 2304
LX = 1


def draw_perambulator(key, part):
    noise_key = jax.random.fold_in(key, 11)
    diag_key = jax.random.fold_in(key, 23)
    shape = (NT, NSTORE, 4, 2, NEV, NEV)
    noise = jax.random.normal(noise_key, shape, jnp.float32) * (0.6 / math.sqrt(NEV))
    diagonal = jnp.exp(jax.random.uniform(diag_key, (NT, NSTORE, 4, NEV), jnp.float32, -0.7, 0.7))
    identity = jnp.eye(NEV, dtype=jnp.float32)
    real_part = noise[:, :, :, 0] + diagonal[:, :, :, :, None] * identity
    return jnp.stack([real_part, noise[:, :, :, 1]], axis=3).astype(jnp.bfloat16)


def draw_source_slots(key, part):
    other_key = jax.random.fold_in(key, 31)
    order_key = jax.random.fold_in(key, 37)
    other = jax.random.randint(other_key, (), 0, NSTORE - 1, jnp.int32)
    last = jnp.full((), NSTORE - 1, jnp.int32)
    order = jax.random.randint(order_key, (), 0, 2, jnp.int32)
    first = jnp.where(order == 0, other, last)
    second = jnp.where(order == 0, last, other)
    return jnp.stack([first, second]).astype(jnp.int32)


def set_ends(result, own_key, low, high):
    longest = result.shape.index(max(result.shape))
    spots = []
    for shift in (0, 1):
        where = [jax.random.randint(jax.random.fold_in(own_key, axis), (), 0, length) for axis, length in enumerate(result.shape)]
        where[longest] = (where[longest] + shift) % result.shape[longest]
        spots.append(tuple(where))
    return result.at[spots[0]].set(low).at[spots[1]].set(high)


def with_spikes(entries, rng, source, target, blocks, factor):
    def block_of(dim):
        return (jnp.arange(entries.shape[dim]) // (entries.shape[dim] // blocks)).reshape((-1,) + (1,) * (entries.ndim - 1 - dim))

    near = jax.random.permutation(rng, blocks)[block_of(target)]
    other_side = (block_of(target) + blocks // 2) % blocks
    return jnp.where((block_of(source) == near) | (block_of(source) == other_side), factor * entries, entries)


def block_levels(own_key, dims, cuts, smallest, largest):
    def one(position, shards_of):
        draws = jax.random.uniform(jax.random.fold_in(jax.random.fold_in(own_key, 6), position), (shards_of,), jnp.float32, smallest / len(cuts), largest / len(cuts))
        return jnp.repeat(jnp.exp(draws), dims[position] // shards_of).reshape((-1,) + (1,) * (len(dims) - position - 1))

    level = one(*cuts[0])
    for cut in cuts[1:]:
        level = level * one(*cut)
    return level


def heavy_noise(key, shape, scale, reach, pieces, heavy, kind=jnp.bfloat16):
    drawn = scale * jax.random.normal(key, shape, jnp.float32)
    if pieces:
        drawn = drawn * block_levels(key, shape, pieces, -0.22, 0.18)
    return jnp.clip(with_spikes(drawn, jax.random.fold_in(key, 3), *heavy), -reach, reach).astype(kind)


def setup_inputs(seed: int = 0, part: int = 0) -> dict:
    key_of = jax.random.split(jax.random.key(seed), 7)
    part_keys = jax.random.split(jax.random.fold_in(key_of[6], part), 7)
    eigvecs = heavy_noise(part_keys[0], (NT, SITES, 3, 2, NEV), 1.0, 6.0, ((0, 2), (1, 8)), (1, 4, 8, 2.0))
    perambulator = draw_perambulator(jax.random.fold_in(jax.random.fold_in(key_of[6], part), 71), part)
    momenta = jax.random.randint(key_of[2], (NMOM, 3), 1, 4).astype(jnp.int32)
    source_slots = draw_source_slots(jax.random.fold_in(key_of[6], 71), part)
    gamma_columns = jax.vmap(lambda own: jax.random.permutation(own, 4))(jax.random.split(key_of[4], NGAM)).reshape((NGAM, 4)).astype(jnp.int32)
    gamma_phases = set_ends(jax.random.randint(key_of[5], (NGAM, 4), 0, 4), jax.random.fold_in(key_of[5], 1), 0, 3).astype(jnp.int32)
    return dict(eigvecs=eigvecs, perambulator=perambulator, momenta=momenta, source_slots=source_slots, gamma_columns=gamma_columns, gamma_phases=gamma_phases)


def gamma_mixer(gamma_columns, gamma_phases):
    spin_ids = jnp.arange(4, dtype=jnp.int32)
    matches = (gamma_columns[:, :, None] == spin_ids[None, None, :]).astype(jnp.float32)
    real_sign = (gamma_phases == 0).astype(jnp.float32) - (gamma_phases == 2).astype(jnp.float32)
    imag_sign = (gamma_phases == 1).astype(jnp.float32) - (gamma_phases == 3).astype(jnp.float32)
    real_part = matches * real_sign[:, :, None]
    imag_part = matches * imag_sign[:, :, None]
    first_row = jnp.stack([real_part, -imag_part], axis=-1)
    second_row = jnp.stack([imag_part, real_part], axis=-1)
    return jnp.stack([first_row, second_row], axis=1)

def apply_gammas(blocks, gamma_mix, factor):
    return factor * jnp.einsum('gostk,apstkb->apgob', gamma_mix, blocks, precision=lax.Precision.HIGHEST)

def phase_tables(momenta, site_ids, extent_x):
    coord_z = site_ids % LZ
    coord_y = site_ids // LZ % LY
    coord_x = site_ids // (LY * LZ)
    turns = (momenta[:, 0:1] * coord_x[None, :] % extent_x).astype(jnp.float32) / extent_x + (momenta[:, 1:2] * coord_y[None, :] % LY).astype(jnp.float32) / LY + (momenta[:, 2:3] * coord_z[None, :] % LZ).astype(jnp.float32) / LZ
    angles = 2.0 * math.pi * turns
    return (jnp.cos(angles), jnp.sin(angles))

def sink_vectors(vectors, picked):
    eig_count = picked.shape[-1]
    real_parts = []
    imag_parts = []
    for spin_index in range(4):
        real_tau = picked[spin_index, 0]
        imag_tau = picked[spin_index, 1]
        stacked = jnp.concatenate([jnp.concatenate([real_tau, imag_tau], axis=1), jnp.concatenate([-imag_tau, real_tau], axis=1)], axis=0)
        product = jnp.dot(vectors, stacked, preferred_element_type=jnp.float32).astype(jnp.bfloat16)
        real_parts.append(product[:, :eig_count])
        imag_parts.append(product[:, eig_count:])
    return (jnp.stack(real_parts, axis=1), jnp.stack(imag_parts, axis=1))

def twisted(right_real, right_imag, cosine, sine):
    moment_count, site_count = cosine.shape
    shaped_real = right_real.astype(jnp.float32).reshape(1, site_count, 3, 4, -1)
    shaped_imag = right_imag.astype(jnp.float32).reshape(1, site_count, 3, 4, -1)
    cosine_wide = cosine.reshape(moment_count, site_count, 1, 1, 1)
    sine_wide = sine.reshape(moment_count, site_count, 1, 1, 1)
    wave_real = (cosine_wide * shaped_real - sine_wide * shaped_imag).astype(jnp.bfloat16)
    wave_imag = (sine_wide * shaped_real + cosine_wide * shaped_imag).astype(jnp.bfloat16)
    return (wave_real.reshape(moment_count, site_count * 3, 4, -1), wave_imag.reshape(moment_count, site_count * 3, 4, -1))

def reference(eigvecs, perambulator, momenta, source_slots, gamma_columns, gamma_phases):
    factor = 1.0 / math.sqrt(12.0 * SITES)
    site_ids = jnp.arange(SITES, dtype=jnp.int32)
    cosine, sine = phase_tables(momenta, site_ids, LX)
    gamma_mix = gamma_mixer(gamma_columns, gamma_phases)
    chosen = jnp.take(perambulator, source_slots.astype(jnp.int32), axis=1)
    row_total = SITES * 3
    results = []
    for time_index in range(NT):
        vectors = eigvecs[time_index].reshape(row_total, 2 * NEV)
        left_real, left_imag = sink_vectors(vectors, chosen[time_index, 0])
        right_real, right_imag = sink_vectors(vectors, chosen[time_index, 1])
        wave_real, wave_imag = twisted(right_real, right_imag, cosine, sine)
        flat_left_real = left_real.reshape(row_total, 4 * NEV)
        flat_left_imag = left_imag.reshape(row_total, 4 * NEV)
        per_momentum = []
        for moment_index in range(NMOM):
            flat_wave_real = wave_real[moment_index].reshape(row_total, 4 * NEV)
            flat_wave_imag = wave_imag[moment_index].reshape(row_total, 4 * NEV)
            real_block = jnp.dot(flat_left_real.T, flat_wave_real, preferred_element_type=jnp.float32) + jnp.dot(flat_left_imag.T, flat_wave_imag, preferred_element_type=jnp.float32)
            imag_block = jnp.dot(flat_left_real.T, flat_wave_imag, preferred_element_type=jnp.float32) - jnp.dot(flat_left_imag.T, flat_wave_real, preferred_element_type=jnp.float32)
            both_parts = jnp.stack([real_block, imag_block], axis=0).reshape(2, 4, NEV, 4, NEV)
            per_momentum.append(both_parts.transpose(2, 1, 3, 0, 4))
        blocks = jnp.stack(per_momentum, axis=1)
        results.append(apply_gammas(blocks, gamma_mix, factor))
    return jnp.stack(results, axis=0)
```

```python
import functools
import math

import jax
import jax.numpy as jnp
from jax import lax
from jax.experimental import pallas as pl
from jax.experimental.pallas import tpu as pltpu
from jax.sharding import PartitionSpec as P

LY = 48
LZ = 48
WIRE = jnp.bfloat16
F32 = jnp.float32
BF16 = jnp.bfloat16
MESH = pl.DeviceIdType.MESH
VMEM_LIMIT = 32 * 1024 * 1024


def site_phases(momenta_at, first_site, site_count, extent_x, shape):
    site = (lax.broadcasted_iota(jnp.int32, shape, 0) + first_site).astype(F32)
    lines = jnp.floor((site + 0.5) * (1.0 / LZ))
    coord_x = jnp.floor((lines + 0.5) * (1.0 / LY))
    coord_y = lines - LY * coord_x
    coord_z = site - LZ * lines

    def share(momentum, coord, extent):
        turn = momentum.astype(F32) * coord * (1.0 / extent)
        return turn - jnp.floor(turn)

    turns = (
        share(momenta_at(0), coord_x, extent_x)
        + share(momenta_at(1), coord_y, LY)
        + share(momenta_at(2), coord_z, LZ)
    )
    turns = turns - jnp.floor(turns + 0.5)
    half = math.pi * turns
    square = half * half
    sine = jnp.full(shape, 1.0 / 6227020800.0, F32)
    for term in (-1.0 / 39916800.0, 1.0 / 362880.0, -1.0 / 5040.0, 1.0 / 120.0, -1.0 / 6.0, 1.0):
        sine = sine * square + term
    sine = sine * half
    cosine = jnp.full(shape, 1.0 / 479001600.0, F32)
    for term in (-1.0 / 3628800.0, 1.0 / 40320.0, -1.0 / 720.0, 1.0 / 24.0, -0.5, 1.0):
        cosine = cosine * square + term
    return 1.0 - 2.0 * sine * sine, 2.0 * sine * cosine


def kernel(
    n, sites, extent_x, factor,
    momenta_hbm, slots_hbm, columns_hbm, phases_hbm, eig_hbm, per_hbm, out_ref,
    momenta, slots, columns, phases, eig, eig32, left, right, per, sink, turned, crossing, picked, wide, part, sums, mfull, mixed, blocks,
    load_sem, own_send, own_recv, fwd_send, fwd_recv,
    turn_send, turn_recv, red_send, red_recv, all_send, all_recv,
):
    me = lax.axis_index("space")
    eig_count = eig.shape[1]
    rows = eig_count // n
    gammas = columns.shape[1]

    load_per = pltpu.make_async_copy(per_hbm, per, load_sem.at[0])
    load_eig = pltpu.make_async_copy(eig_hbm, eig, load_sem.at[1])
    load_slots = pltpu.make_async_copy(slots_hbm, slots, load_sem.at[2])
    load_momenta = pltpu.make_async_copy(momenta_hbm, momenta, load_sem.at[3])
    load_columns = pltpu.make_async_copy(columns_hbm, columns, load_sem.at[4])
    load_phases = pltpu.make_async_copy(phases_hbm, phases, load_sem.at[5])
    for load in (load_eig, load_momenta, load_slots, load_per, load_columns, load_phases):
        load.start()

    hubs = n // 2
    hub_rows = eig_count // hubs
    slot = me - n // 4
    is_hub = (slot >= 0) & (slot < hubs)
    side = lax.rem(me, 2)
    partner = me + 1 - 2 * side
    corner = n - 1 - me

    barrier = pltpu.get_barrier_semaphore()

    def greet(peer):
        pl.semaphore_signal(barrier, inc=1, device_id={"space": peer}, device_id_type=MESH)

    for k in range(1, n):
        peer = lax.rem(me + k, n)
        pl.when(is_hub | (peer != corner))(functools.partial(greet, peer))

    load_slots.wait()
    load_per.wait()
    mine = pl.ds(pl.multiple_of(me * rows, rows), rows)
    sink[:, :, mine, :] = per[slots[1]]
    first = per[slots[0]].reshape(8 * rows, eig_count).astype(F32)
    turned[...] = first.T.astype(BF16).reshape(n, rows, 8 * rows)

    def remote(src, dst, send, recv, peer):
        return pltpu.make_async_remote_copy(
            src_ref=src, dst_ref=dst, send_sem=send, recv_sem=recv,
            device_id={"space": peer}, device_id_type=MESH,
        )

    def sink_of(owner):
        return sink.at[:, :, pl.ds(pl.multiple_of(owner * rows, rows), rows), :]

    load_momenta.wait()
    load_eig.wait()
    eig32[...] = eig[...].astype(F32)
    cosine, sine = site_phases(lambda i: momenta[0, i], me * sites, sites, extent_x, (sites, eig_count))
    for color in range(3):
        real = eig32[pl.ds(2 * color, sites, stride=6), :]
        imag = eig32[pl.ds(2 * color + 1, sites, stride=6), :]
        wave_real = (cosine * real - sine * imag).astype(BF16)
        wave_imag = (sine * real + cosine * imag).astype(BF16)
        low = pl.ds(2 * color * sites, sites)
        high = pl.ds((2 * color + 1) * sites, sites)
        left[low, :] = real.astype(BF16)
        left[high, :] = imag.astype(BF16)
        right[low, :eig_count] = wave_real
        right[low, eig_count:] = wave_imag
        right[high, :eig_count] = wave_imag
        right[high, eig_count:] = -wave_real
    whole = lax.dot_general(
        left[...], right[...], (((0,), (0,)), ((), ())), preferred_element_type=F32
    )
    part[...] = whole.astype(part.dtype).reshape(hubs, hub_rows, 2 * eig_count)

    pl.semaphore_wait(barrier, n - 2 + is_hub.astype(jnp.int32))

    def red(j):
        return remote(part.at[j], sums.at[me], red_send.at[j], red_recv.at[me], j + n // 4)

    for i in range(hubs):
        j = jnp.where(me < n // 2, hubs - 1 - i, i)
        pl.when(slot != j)(functools.partial(lambda j: red(j).start(), j))

    near = remote(sink_of(me), sink_of(me), own_send.at[0], own_recv.at[0], partner)
    near_turn = remote(turned.at[partner], picked.at[me], turn_send.at[0], turn_recv.at[0], partner)
    line = lax.div(me, 2)
    lines = n // 2
    lower = line < lines // 2
    mirror = jnp.where(lower, line, lines - 1 - line)

    def other_line(k):
        far = lines - 1 - k
        far = far - (far <= mirror).astype(jnp.int32)
        return jnp.where(lower, far, lines - 1 - far)

    def cross(k, target, origin):
        peer = 2 * target + side
        pair = pl.ds(pl.multiple_of(2 * target, 2), 2)
        owner = 2 * origin + side
        return (
            remote(
                turned.at[pair], crossing.at[origin], turn_send.at[1 + k],
                turn_recv.at[1 + origin], peer,
            ),
            remote(
                sink_of(owner), sink_of(owner), own_send.at[1 + k], own_recv.at[1 + origin], peer
            ),
        )

    own = []
    for k in range(lines - 1):
        own.extend(cross(k, other_line(k), line))
    for copy in [near_turn] + own + [near]:
        copy.start()

    def gather(k):
        peer = lax.rem(me + k, n)
        here = jnp.clip(slot, 0, hubs - 1)
        return remote(mfull.at[here], mfull.at[here], all_send.at[k], all_recv.at[here], peer)

    @pl.when(is_hub)
    def _():
        total = part[jnp.clip(slot, 0, hubs - 1)].astype(F32)
        for k in range(1, n):
            source = lax.rem(me + k, n)
            remote(part.at[0], sums.at[source], red_send.at[0], red_recv.at[source], source).wait_recv()
            total = total + sums[source].astype(F32)
        mfull[jnp.clip(slot, 0, hubs - 1)] = total.astype(BF16)
        for k in range(1, n):
            gather(k).start()

    fwds = []
    for k in range(lines - 1):
        origin = other_line(lines - 2 - k)
        for copy in cross(0, origin, origin):
            copy.wait_recv()
        owner = 2 * origin + side
        fwds.append(
            remote(
                crossing.at[origin, 1 - side], picked.at[owner],
                fwd_send.at[k + lines], fwd_recv.at[origin + lines], partner,
            )
        )
        fwds.append(
            remote(sink_of(owner), sink_of(owner), fwd_send.at[k], fwd_recv.at[origin], partner)
        )
        fwds[-2].start()
        fwds[-1].start()
        picked[owner] = crossing[origin, side]
    picked[me] = turned[me]
    near_turn.wait_recv()
    near.wait_recv()
    for copy in fwds:
        copy.wait_recv()

    load_columns.wait()
    load_phases.wait()
    spin_of = lax.broadcasted_iota(jnp.int32, (rows, 8 * rows), 1) // (2 * rows)
    for k in range(n):
        block = picked[k].astype(F32)
        for spin in range(4):
            wide[pl.ds(spin * rows, rows), pl.ds(k * 8 * rows, 8 * rows)] = jnp.where(
                spin_of == spin, block, 0.0
            ).astype(BF16)
    for j in range(hubs):
        arrival = remote(mfull.at[j], mfull.at[j], all_send.at[0], all_recv.at[j], partner)
        pl.when(slot != j)(arrival.wait_recv)
        for half in range(2):
            block = mfull[j, half * rows : (half + 1) * rows]
            turned_block = jnp.concatenate([block[:, eig_count:], -block[:, :eig_count]], axis=1)
            for spin in range(4):
                base = (2 * j + half) * 8 * rows + spin * 2 * rows
                mixed[pl.ds(base, rows), :] = block
                mixed[pl.ds(base + rows, rows), :] = turned_block
    cross = jnp.dot(wide[...], mixed[...], preferred_element_type=F32)
    cross_real, cross_imag = cross[:, :eig_count], cross[:, eig_count:]
    stacked = jnp.concatenate(
        [
            jnp.concatenate([cross_real, -cross_imag], axis=1),
            jnp.concatenate([cross_imag, cross_real], axis=1),
        ],
        axis=0,
    ).astype(BF16)
    for pair in range(2):
        table = jnp.concatenate(
            [sink[2 * pair + i].reshape(2 * eig_count, eig_count) for i in range(2)], axis=1
        )
        result = jnp.dot(stacked, table, preferred_element_type=F32) * factor
        for i in range(2):
            for half in range(2):
                for spin in range(4):
                    base = (half * 4 + spin) * rows
                    blocks[half, spin * 4 + 2 * pair + i] = result[
                        base : base + rows, i * eig_count : (i + 1) * eig_count
                    ]
    for g in range(gammas):
        real = imag = None
        for spin in range(4):
            phase = phases[spin, g]
            odd = phase % 2
            index = spin * 4 + columns[spin, g]
            sign_real = jnp.where((phase == 0) | (phase == 3), 1.0, -1.0).astype(F32)
            sign_imag = jnp.where(phase < 2, 1.0, -1.0).astype(F32)
            term_real = sign_real * blocks[odd, index]
            term_imag = sign_imag * blocks[1 - odd, index]
            real = term_real if real is None else real + term_real
            imag = term_imag if imag is None else imag + term_imag
        out_ref[pl.ds(2 * g, rows, stride=2 * gammas), :] = real
        out_ref[pl.ds(2 * g + 1, rows, stride=2 * gammas), :] = imag

    for copy in own + fwds + [near, near_turn]:
        copy.wait_send()
    for j in range(hubs):
        pl.when(slot != j)(lambda j=j: red(j).wait_send())

    @pl.when(is_hub)
    def _():
        for k in range(1, n):
            gather(k).wait_send()


def store_kernel(source, target, sem):
    copy = pltpu.make_async_copy(source, target, sem.at[0])
    copy.start()
    copy.wait()


def on_device_kernel(eigvecs, perambulator, momenta, source_slots, gamma_columns, gamma_phases):
    sites, eig_count = eigvecs.shape[1], eigvecs.shape[4]
    n = lax.axis_size("space")
    rows = eig_count // n
    total_sites = sites * n
    gammas = gamma_columns.shape[0]
    stored = perambulator.shape[1]
    body = functools.partial(
        kernel, n, sites, total_sites // (LY * LZ), 1.0 / math.sqrt(12.0 * total_sites)
    )
    dma = pltpu.SemaphoreType.DMA
    hbm = pl.BlockSpec(memory_space=pltpu.HBM)
    out = pl.pallas_call(
        body,
        out_shape=pltpu.VMEM((rows * gammas * 2, eig_count), F32),
        in_specs=[hbm] * 6,
        out_specs=pl.BlockSpec(memory_space=pltpu.VMEM),
        scratch_shapes=[
            pltpu.SMEM(momenta.shape, jnp.int32),
            pltpu.SMEM(source_slots.shape, jnp.int32),
            pltpu.SMEM((4, gammas), jnp.int32),
            pltpu.SMEM((4, gammas), jnp.int32),
            pltpu.VMEM((sites * 6, eig_count), BF16),
            pltpu.VMEM((sites * 6, eig_count), F32),
            pltpu.VMEM((sites * 6, eig_count), BF16),
            pltpu.VMEM((sites * 6, 2 * eig_count), BF16),
            pltpu.VMEM((stored, 4, 2, rows, eig_count), BF16),
            pltpu.VMEM((4, 2, eig_count, eig_count), BF16),
            pltpu.VMEM((n, rows, 8 * rows), BF16),
            pltpu.VMEM((n // 2, 2, rows, 8 * rows), BF16),
            pltpu.VMEM((n, rows, 8 * rows), BF16),
            pltpu.VMEM((4 * rows, 8 * eig_count), BF16),
            pltpu.VMEM((n // 2, 2 * rows, 2 * eig_count), WIRE),
            pltpu.VMEM((n, 2 * rows, 2 * eig_count), WIRE),
            pltpu.VMEM((n // 2, 2 * rows, 2 * eig_count), BF16),
            pltpu.VMEM((8 * eig_count, 2 * eig_count), BF16),
            pltpu.VMEM((2, 16, rows, eig_count), F32),
            dma((6,)),
        ]
        + [dma((n,)) for _ in range(10)],
        compiler_params=pltpu.CompilerParams(
            collective_id=0, has_side_effects=True, vmem_limit_bytes=VMEM_LIMIT
        ),
    )(
        *(
            pltpu.with_memory_space_constraint(array, pltpu.HBM)
            for array in (
                momenta,
                source_slots,
                gamma_columns.T,
                gamma_phases.T,
                eigvecs.reshape(sites * 6, eig_count),
                perambulator[0],
            )
        )
    )
    done = pl.pallas_call(
        store_kernel,
        out_shape=jax.ShapeDtypeStruct(out.shape, F32),
        in_specs=[pl.BlockSpec(memory_space=pl.ANY)],
        out_specs=hbm,
        scratch_shapes=[dma((1,))],
        compiler_params=pltpu.CompilerParams(vmem_limit_bytes=VMEM_LIMIT),
    )(out)
    return done.reshape(1, rows, 1, gammas, 2, eig_count)


def on_device_plain(eigvecs, perambulator, momenta, source_slots, gamma_columns, gamma_phases):
    sites, eig_count = eigvecs.shape[1], eigvecs.shape[4]
    n = lax.axis_size("space")
    total_sites = sites * n
    extent_x = total_sites // (LY * LZ)
    factor = 1.0 / math.sqrt(12.0 * total_sites)
    first_site = lax.axis_index("space") * sites
    chosen = jnp.take(perambulator[0], source_slots, axis=0)
    sinks = lax.all_gather(chosen[1], "space", axis=2, tiled=True)
    turned = lax.all_to_all(chosen[0], "space", split_axis=3, concat_axis=2, tiled=True)
    real = eigvecs[0, :, :, 0].astype(F32)
    imag = eigvecs[0, :, :, 1].astype(F32)
    flat = eigvecs[0].reshape(sites * 6, eig_count)
    tables = []
    for p in range(momenta.shape[0]):
        cosine, sine = site_phases(
            lambda i, p=p: momenta[p, i], first_site, sites, extent_x, (sites, 1, 1)
        )
        wave_real = cosine * real - sine * imag
        wave_imag = sine * real + cosine * imag
        upper = jnp.concatenate([wave_real, wave_imag], axis=2)
        lower = jnp.concatenate([wave_imag, -wave_real], axis=2)
        waves = jnp.stack([upper, lower], axis=2).astype(BF16).reshape(sites * 6, 2 * eig_count)
        tables.append(
            lax.dot_general(flat, waves, (((0,), (0,)), ((), ())), preferred_element_type=F32)
        )
    whole = lax.psum(jnp.stack(tables), "space").astype(BF16)
    turned_whole = jnp.concatenate([whole[:, :, eig_count:], -whole[:, :, :eig_count]], axis=2)
    both = jnp.stack([whole, turned_whole], axis=1)
    cross = jnp.einsum("skla,pklm->aspm", turned, both, preferred_element_type=F32)
    cross_real, cross_imag = cross[..., :eig_count], cross[..., eig_count:]
    stacked = jnp.stack(
        [
            jnp.stack([cross_real, -cross_imag], axis=-2),
            jnp.stack([cross_imag, cross_real], axis=-2),
        ],
        axis=3,
    ).astype(BF16)
    blocks = jnp.einsum("asphkl,tklb->apsthb", stacked, sinks, preferred_element_type=F32)
    spins = jnp.arange(4, dtype=jnp.int32)
    matches = (gamma_columns[:, :, None] == spins).astype(F32)
    real_sign = (gamma_phases == 0).astype(F32) - (gamma_phases == 2).astype(F32)
    imag_sign = (gamma_phases == 1).astype(F32) - (gamma_phases == 3).astype(F32)
    mix_real = matches * real_sign[:, :, None]
    mix_imag = matches * imag_sign[:, :, None]
    mix = jnp.stack(
        [jnp.stack([mix_real, -mix_imag], axis=-1), jnp.stack([mix_imag, mix_real], axis=-1)],
        axis=1,
    )
    meson = factor * jnp.einsum("gosth,apsthb->apgob", mix, blocks, precision=lax.Precision.HIGHEST)
    return meson[None]


def on_device(eigvecs, perambulator, momenta, *rest):
    n = lax.axis_size("space")
    rows = perambulator.shape[4]
    small = eigvecs.shape[1] % 16 == 0 and eigvecs.shape[4] == 128
    if rows % 16 == 0 and n % 4 == 0 and momenta.shape[0] == 1 and small:
        return on_device_kernel(eigvecs, perambulator, momenta, *rest)
    return on_device_plain(eigvecs, perambulator, momenta, *rest)


def solution(mesh):
    in_specs = (
        P(("cfg", "tm"), "space", None, None, None),
        P(("cfg", "tm"), None, None, None, "space", None),
        P(),
        P(),
        P(),
        P(),
    )
    out_specs = P(("cfg", "tm"), "space", None, None, None, None)
    return jax.shard_map(
        on_device, mesh=mesh, in_specs=in_specs, out_specs=out_specs, check_vma=False
    )
```

```python
import functools
import math

import jax
import jax.numpy as jnp
from jax import lax
from jax.experimental import pallas as pl
from jax.experimental.pallas import tpu as pltpu
from jax.sharding import PartitionSpec as P

LY = 48
LZ = 48
WIRE = jnp.bfloat16
F32 = jnp.float32
BF16 = jnp.bfloat16
MESH = pl.DeviceIdType.MESH
VMEM_LIMIT = 32 * 1024 * 1024


def site_phases(momenta_at, first_site, site_count, extent_x, shape):
    site = (lax.broadcasted_iota(jnp.int32, shape, 0) + first_site).astype(F32)
    lines = jnp.floor((site + 0.5) * (1.0 / LZ))
    coord_x = jnp.floor((lines + 0.5) * (1.0 / LY))
    coord_y = lines - LY * coord_x
    coord_z = site - LZ * lines

    def share(momentum, coord, extent):
        turn = momentum.astype(F32) * coord * (1.0 / extent)
        return turn - jnp.floor(turn)

    turns = (
        share(momenta_at(0), coord_x, extent_x)
        + share(momenta_at(1), coord_y, LY)
        + share(momenta_at(2), coord_z, LZ)
    )
    turns = turns - jnp.floor(turns + 0.5)
    half = math.pi * turns
    square = half * half
    sine = jnp.full(shape, 1.0 / 6227020800.0, F32)
    for term in (-1.0 / 39916800.0, 1.0 / 362880.0, -1.0 / 5040.0, 1.0 / 120.0, -1.0 / 6.0, 1.0):
        sine = sine * square + term
    sine = sine * half
    cosine = jnp.full(shape, 1.0 / 479001600.0, F32)
    for term in (-1.0 / 3628800.0, 1.0 / 40320.0, -1.0 / 720.0, 1.0 / 24.0, -0.5, 1.0):
        cosine = cosine * square + term
    return 1.0 - 2.0 * sine * sine, 2.0 * sine * cosine


def kernel(
    n, sites, extent_x, factor,
    momenta_hbm, slots_hbm, columns_hbm, phases_hbm, eig_hbm, per_hbm, out_ref,
    momenta, slots, columns, phases, eig, eig32, waves, left, right, per, sink, turned, picked,
    part, sums, mfull, blocks, volume,
    load_sem, send_sem, red_recv, all_recv, turn_recv, near_recv, line_recv,
):
    me = lax.axis_index("space")
    eig_count = eig.shape[1]
    rows = eig_count // n
    gammas = columns.shape[1]
    hubs = n // 2
    hub_rows = eig_count // hubs
    slot = me - n // 4
    is_hub = (slot >= 0) & (slot < hubs)
    here = jnp.clip(slot, 0, hubs - 1)
    side = lax.rem(me, 2)
    line = lax.div(me, 2)
    lines = n // 2
    partner = me + 1 - 2 * side

    load_per = pltpu.make_async_copy(per_hbm, per, load_sem.at[0])
    load_eig = pltpu.make_async_copy(eig_hbm, eig, load_sem.at[1])
    load_slots = pltpu.make_async_copy(slots_hbm, slots, load_sem.at[2])
    load_momenta = pltpu.make_async_copy(momenta_hbm, momenta, load_sem.at[3])
    load_columns = pltpu.make_async_copy(columns_hbm, columns, load_sem.at[4])
    load_phases = pltpu.make_async_copy(phases_hbm, phases, load_sem.at[5])
    for load in (load_slots, load_momenta, load_per, load_eig, load_columns, load_phases):
        load.start()

    barrier = pltpu.get_barrier_semaphore()
    for k in range(1, n):
        pl.semaphore_signal(
            barrier, inc=1, device_id={"space": lax.rem(me + k, n)}, device_id_type=MESH
        )

    def remote(src, dst, recv, peer):
        return pltpu.make_async_remote_copy(
            src_ref=src, dst_ref=dst, send_sem=send_sem.at[0], recv_sem=recv,
            device_id={"space": peer}, device_id_type=MESH,
        )

    def arrived(ref, sem):
        pltpu.make_async_copy(ref, ref, sem).wait()

    def sink_of(owner):
        return sink.at[:, :, pl.ds(pl.multiple_of(owner * rows, rows), rows), :]

    def other_line(k):
        lower = line < lines // 2
        mirror = jnp.where(lower, line, lines - 1 - line)
        near = k + (k >= mirror).astype(jnp.int32)
        return jnp.where(lower, near, lines - 1 - near)

    def send_sink(target):
        remote(sink_of(me), sink_of(me), line_recv.at[line], 2 * target + side).start()

    def send_near():
        remote(sink_of(me), sink_of(me), near_recv.at[0], partner).start()

    load_slots.wait()
    load_per.wait()
    mine = pl.ds(pl.multiple_of(me * rows, rows), rows)
    sink[:, :, mine, :] = per[slots[1]]
    first = per[slots[0]].reshape(8 * rows, eig_count).astype(F32)
    turned[...] = first.T.astype(BF16).reshape(n, rows, 8 * rows)
    picked[me] = turned[me]

    load_momenta.wait()
    cosine, sine = site_phases(lambda i: momenta[0, i], me * sites, sites, extent_x, (sites, eig_count))
    waves[0] = cosine
    waves[1] = sine

    load_eig.wait()
    eig32[...] = eig[...].astype(F32)
    for color in range(3):
        real = eig32[pl.ds(2 * color, sites, stride=6), :]
        imag = eig32[pl.ds(2 * color + 1, sites, stride=6), :]
        wave_real = (waves[0] * real - waves[1] * imag).astype(BF16)
        wave_imag = (waves[1] * real + waves[0] * imag).astype(BF16)
        low = pl.ds(2 * color * sites, sites)
        high = pl.ds((2 * color + 1) * sites, sites)
        left[low, :] = real.astype(BF16)
        left[high, :] = imag.astype(BF16)
        right[low, :eig_count] = wave_real
        right[low, eig_count:] = wave_imag
        right[high, :eig_count] = wave_imag
        right[high, eig_count:] = -wave_real
    whole = lax.dot_general(
        left[...], right[...], (((0,), (0,)), ((), ())), preferred_element_type=F32
    )
    part[...] = whole.astype(part.dtype).reshape(hubs, hub_rows, 2 * eig_count)

    def send_red():
        for i in range(hubs):
            j = jnp.where(me < n // 2, hubs - 1 - i, i)
            pl.when(slot != j)(
                lambda j=j: remote(part.at[j], sums.at[me], red_recv.at[0], j + n // 4).start()
            )

    def send_turned():
        for k in range(1, n):
            peer = lax.rem(me + k, n)
            remote(turned.at[peer], picked.at[me], turn_recv.at[0], peer).start()

    pl.semaphore_wait(barrier, n - 1)
    send_red()
    send_near()
    for k in reversed(range(lines - 1)):
        send_sink(other_line(k))
    send_turned()

    @pl.when(is_hub)
    def _():
        arrived(sums.at[pl.ds(0, n - 1)], red_recv.at[0])
        total = part[here].astype(F32)
        for k in range(1, n):
            total = total + sums[lax.rem(me + k, n)].astype(F32)
        mfull[here] = total.astype(BF16)
        for k in range(1, n):
            peer = k - 1 + (k - 1 >= me).astype(jnp.int32)
            remote(mfull.at[here], mfull.at[here], all_recv.at[0], peer).start()

    for k in range(lines - 1):
        origin = other_line(k)
        owner = 2 * origin + side
        arrived(sink_of(owner), line_recv.at[origin])
        remote(sink_of(owner), sink_of(owner), near_recv.at[0], partner).start()

    arrived(picked.at[pl.ds(0, n - 1)], turn_recv.at[0])
    group = lax.broadcasted_iota(jnp.int32, (rows, eig_count), 1) // rows
    chunks = [None] * 8
    for k in range(n):
        block = picked[k].astype(F32)
        for c in range(8):
            turn = (k - c) % 8
            moved = pltpu.roll(block, turn * rows, 1) if turn else block
            chunks[c] = moved if chunks[c] is None else jnp.where(group == k, moved, chunks[c])
    sources = jnp.concatenate(chunks[0::2] + chunks[1::2], axis=0).astype(BF16)
    load_columns.wait()
    load_phases.wait()
    arrived(sink.at[:, :, pl.ds(0, lines * rows), :], near_recv.at[0])

    @pl.when(is_hub)
    def _():
        arrived(mfull.at[pl.ds(0, hubs - 1)], all_recv.at[0])

    @pl.when(jnp.logical_not(is_hub))
    def _():
        arrived(mfull, all_recv.at[0])

    half = 4 * rows
    both = jnp.dot(sources, mfull[...].reshape(eig_count, 2 * eig_count), preferred_element_type=F32)
    cross_real = ((both[:half, :eig_count] + both[half:, eig_count:]) * factor).astype(BF16)
    cross_imag = ((both[:half, eig_count:] - both[half:, :eig_count]) * factor).astype(BF16)
    stacked = jnp.concatenate(
        [
            jnp.concatenate([cross_real, -cross_imag], axis=1),
            jnp.concatenate([cross_imag, cross_real], axis=1),
        ],
        axis=0,
    )
    for pair in range(2):
        table = jnp.concatenate(
            [sink[2 * pair + i].reshape(2 * eig_count, eig_count) for i in range(2)], axis=1
        )
        result = jnp.dot(stacked, table, preferred_element_type=F32)
        for i in range(2):
            for part_of in range(2):
                for spin in range(4):
                    base = (part_of * 4 + spin) * rows
                    blocks[part_of, spin * 4 + 2 * pair + i] = result[
                        base : base + rows, i * eig_count : (i + 1) * eig_count
                    ]
    for g in range(gammas):
        real = imag = None
        for spin in range(4):
            phase = phases[spin, g]
            odd = phase % 2
            index = spin * 4 + columns[spin, g]
            sign_real = jnp.where((phase == 0) | (phase == 3), 1.0, -1.0).astype(F32)
            sign_imag = jnp.where(phase < 2, 1.0, -1.0).astype(F32)
            term_real = sign_real * blocks[odd, index]
            term_imag = sign_imag * blocks[1 - odd, index]
            real = term_real if real is None else real + term_real
            imag = term_imag if imag is None else imag + term_imag
        out_ref[pl.ds(2 * g, rows, stride=2 * gammas), :] = real
        out_ref[pl.ds(2 * g + 1, rows, stride=2 * gammas), :] = imag

    unit = 4 * rows
    plain = hubs * unit + 2 * lines * 8 * rows + (n - 1) * rows - 8 * rows
    extra = (hubs - 1 + n - 1 - hubs) * unit

    @pl.when(is_hub)
    def _():
        arrived(volume.at[pl.ds(0, plain + extra)], send_sem.at[0])

    @pl.when(jnp.logical_not(is_hub))
    def _():
        arrived(volume.at[pl.ds(0, plain)], send_sem.at[0])


def store_kernel(source, target, sem):
    copy = pltpu.make_async_copy(source, target, sem.at[0])
    copy.start()
    copy.wait()


def on_device_kernel(eigvecs, perambulator, momenta, source_slots, gamma_columns, gamma_phases):
    sites, eig_count = eigvecs.shape[1], eigvecs.shape[4]
    n = lax.axis_size("space")
    rows = eig_count // n
    total_sites = sites * n
    gammas = gamma_columns.shape[0]
    stored = perambulator.shape[1]
    body = functools.partial(
        kernel, n, sites, total_sites // (LY * LZ), 1.0 / math.sqrt(12.0 * total_sites)
    )
    dma = pltpu.SemaphoreType.DMA
    hbm = pl.BlockSpec(memory_space=pltpu.HBM)
    out = pl.pallas_call(
        body,
        out_shape=pltpu.VMEM((rows * gammas * 2, eig_count), F32),
        in_specs=[hbm] * 6,
        out_specs=pl.BlockSpec(memory_space=pltpu.VMEM),
        scratch_shapes=[
            pltpu.SMEM(momenta.shape, jnp.int32),
            pltpu.SMEM(source_slots.shape, jnp.int32),
            pltpu.SMEM((4, gammas), jnp.int32),
            pltpu.SMEM((4, gammas), jnp.int32),
            pltpu.VMEM((sites * 6, eig_count), BF16),
            pltpu.VMEM((sites * 6, eig_count), F32),
            pltpu.VMEM((2, sites, eig_count), F32),
            pltpu.VMEM((sites * 6, eig_count), BF16),
            pltpu.VMEM((sites * 6, 2 * eig_count), BF16),
            pltpu.VMEM((stored, 4, 2, rows, eig_count), BF16),
            pltpu.VMEM((4, 2, eig_count, eig_count), BF16),
            pltpu.VMEM((n, rows, 8 * rows), BF16),
            pltpu.VMEM((n, rows, 8 * rows), BF16),
            pltpu.VMEM((n // 2, 2 * rows, 2 * eig_count), WIRE),
            pltpu.VMEM((n, 2 * rows, 2 * eig_count), WIRE),
            pltpu.VMEM((n // 2, 2 * rows, 2 * eig_count), BF16),
            pltpu.VMEM((2, 16, rows, eig_count), F32),
            pltpu.VMEM((16 * eig_count, eig_count), BF16),
            dma((6,)),
            dma((1,)),
            dma((1,)),
            dma((1,)),
            dma((1,)),
            dma((1,)),
            dma((n // 2,)),
        ],
        compiler_params=pltpu.CompilerParams(
            collective_id=0, has_side_effects=True, vmem_limit_bytes=VMEM_LIMIT
        ),
    )(
        *(
            pltpu.with_memory_space_constraint(array, pltpu.HBM)
            for array in (
                momenta,
                source_slots,
                gamma_columns.T,
                gamma_phases.T,
                eigvecs.reshape(sites * 6, eig_count),
                perambulator[0],
            )
        )
    )
    done = pl.pallas_call(
        store_kernel,
        out_shape=jax.ShapeDtypeStruct(out.shape, F32),
        in_specs=[pl.BlockSpec(memory_space=pl.ANY)],
        out_specs=hbm,
        scratch_shapes=[dma((1,))],
        compiler_params=pltpu.CompilerParams(vmem_limit_bytes=VMEM_LIMIT),
    )(out)
    return done.reshape(1, rows, 1, gammas, 2, eig_count)


def on_device_plain(eigvecs, perambulator, momenta, source_slots, gamma_columns, gamma_phases):
    sites, eig_count = eigvecs.shape[1], eigvecs.shape[4]
    n = lax.axis_size("space")
    total_sites = sites * n
    extent_x = total_sites // (LY * LZ)
    factor = 1.0 / math.sqrt(12.0 * total_sites)
    first_site = lax.axis_index("space") * sites
    chosen = jnp.take(perambulator[0], source_slots, axis=0)
    sinks = lax.all_gather(chosen[1], "space", axis=2, tiled=True)
    turned = lax.all_to_all(chosen[0], "space", split_axis=3, concat_axis=2, tiled=True)
    real = eigvecs[0, :, :, 0].astype(F32)
    imag = eigvecs[0, :, :, 1].astype(F32)
    flat = eigvecs[0].reshape(sites * 6, eig_count)
    tables = []
    for p in range(momenta.shape[0]):
        cosine, sine = site_phases(
            lambda i, p=p: momenta[p, i], first_site, sites, extent_x, (sites, 1, 1)
        )
        wave_real = cosine * real - sine * imag
        wave_imag = sine * real + cosine * imag
        upper = jnp.concatenate([wave_real, wave_imag], axis=2)
        lower = jnp.concatenate([wave_imag, -wave_real], axis=2)
        waves = jnp.stack([upper, lower], axis=2).astype(BF16).reshape(sites * 6, 2 * eig_count)
        tables.append(
            lax.dot_general(flat, waves, (((0,), (0,)), ((), ())), preferred_element_type=F32)
        )
    whole = lax.psum(jnp.stack(tables), "space").astype(BF16)
    turned_whole = jnp.concatenate([whole[:, :, eig_count:], -whole[:, :, :eig_count]], axis=2)
    both = jnp.stack([whole, turned_whole], axis=1)
    cross = jnp.einsum("skla,pklm->aspm", turned, both, preferred_element_type=F32)
    cross_real, cross_imag = cross[..., :eig_count], cross[..., eig_count:]
    stacked = jnp.stack(
        [
            jnp.stack([cross_real, -cross_imag], axis=-2),
            jnp.stack([cross_imag, cross_real], axis=-2),
        ],
        axis=3,
    ).astype(BF16)
    blocks = jnp.einsum("asphkl,tklb->apsthb", stacked, sinks, preferred_element_type=F32)
    spins = jnp.arange(4, dtype=jnp.int32)
    matches = (gamma_columns[:, :, None] == spins).astype(F32)
    real_sign = (gamma_phases == 0).astype(F32) - (gamma_phases == 2).astype(F32)
    imag_sign = (gamma_phases == 1).astype(F32) - (gamma_phases == 3).astype(F32)
    mix_real = matches * real_sign[:, :, None]
    mix_imag = matches * imag_sign[:, :, None]
    mix = jnp.stack(
        [jnp.stack([mix_real, -mix_imag], axis=-1), jnp.stack([mix_imag, mix_real], axis=-1)],
        axis=1,
    )
    meson = factor * jnp.einsum("gosth,apsthb->apgob", mix, blocks, precision=lax.Precision.HIGHEST)
    return meson[None]


def on_device(eigvecs, perambulator, momenta, *rest):
    n = lax.axis_size("space")
    rows = perambulator.shape[4]
    small = eigvecs.shape[1] % 16 == 0 and eigvecs.shape[4] == 128
    if rows == 16 and n == 8 and momenta.shape[0] == 1 and small:
        return on_device_kernel(eigvecs, perambulator, momenta, *rest)
    return on_device_plain(eigvecs, perambulator, momenta, *rest)


def solution(mesh):
    in_specs = (
        P(("cfg", "tm"), "space", None, None, None),
        P(("cfg", "tm"), None, None, None, "space", None),
        P(),
        P(),
        P(),
        P(),
    )
    out_specs = P(("cfg", "tm"), "space", None, None, None, None)
    return jax.shard_map(
        on_device, mesh=mesh, in_specs=in_specs, out_specs=out_specs, check_vma=False
    )
```

```python
import functools
import math

import jax
import jax.numpy as jnp
from jax import lax
from jax.experimental import pallas as pl
from jax.experimental.pallas import tpu as pltpu
from jax.sharding import PartitionSpec as P

LY = 48
LZ = 48
WIRE = jnp.bfloat16
F32 = jnp.float32
BF16 = jnp.bfloat16
MESH = pl.DeviceIdType.MESH
VMEM_LIMIT = 32 * 1024 * 1024


def site_phases(momenta_at, first_site, site_count, extent_x, shape):
    site = (lax.broadcasted_iota(jnp.int32, shape, 0) + first_site).astype(F32)
    lines = jnp.floor((site + 0.5) * (1.0 / LZ))
    coord_x = jnp.floor((lines + 0.5) * (1.0 / LY))
    coord_y = lines - LY * coord_x
    coord_z = site - LZ * lines

    def share(momentum, coord, extent):
        turn = momentum.astype(F32) * coord * (1.0 / extent)
        return turn - jnp.floor(turn)

    turns = (
        share(momenta_at(0), coord_x, extent_x)
        + share(momenta_at(1), coord_y, LY)
        + share(momenta_at(2), coord_z, LZ)
    )
    turns = turns - jnp.floor(turns + 0.5)
    half = math.pi * turns
    square = half * half
    sine = jnp.full(shape, 1.0 / 6227020800.0, F32)
    for term in (-1.0 / 39916800.0, 1.0 / 362880.0, -1.0 / 5040.0, 1.0 / 120.0, -1.0 / 6.0, 1.0):
        sine = sine * square + term
    sine = sine * half
    cosine = jnp.full(shape, 1.0 / 479001600.0, F32)
    for term in (-1.0 / 3628800.0, 1.0 / 40320.0, -1.0 / 720.0, 1.0 / 24.0, -0.5, 1.0):
        cosine = cosine * square + term
    return 1.0 - 2.0 * sine * sine, 2.0 * sine * cosine


def kernel(
    n, sites, extent_x, factor,
    momenta_hbm, slots_hbm, columns_hbm, phases_hbm, eig_hbm, per_hbm, out_ref,
    momenta, slots, columns, phases, eig, eig32, waves, left, right, per, sink, turned, picked,
    part, sums, spread, mfull, blocks, volume,
    ready, reply, load_sem, send_sem, red_recv, all_recv, turn_recv, near_recv, line_recv,
):
    me = lax.axis_index("space")
    time = lax.axis_index("tm")
    times = lax.axis_size("tm")
    hub_time = times - 1
    eig_count = eig.shape[1]
    rows = eig_count // n
    gammas = columns.shape[1]
    hubs = n // 2
    hub_rows = eig_count // hubs
    slot = me - n // 4
    inner = (slot >= 0) & (slot < hubs)
    is_hub = inner & (time == hub_time)
    is_leaf = jnp.logical_not(is_hub)
    here = jnp.clip(slot, 0, hubs - 1)
    side = lax.rem(me, 2)
    line = lax.div(me, 2)
    lines = n // 2
    partner = me + 1 - 2 * side

    load_per = pltpu.make_async_copy(per_hbm, per, load_sem.at[0])
    load_eig = pltpu.make_async_copy(eig_hbm, eig, load_sem.at[1])
    load_slots = pltpu.make_async_copy(slots_hbm, slots, load_sem.at[2])
    load_momenta = pltpu.make_async_copy(momenta_hbm, momenta, load_sem.at[3])
    load_columns = pltpu.make_async_copy(columns_hbm, columns, load_sem.at[4])
    load_phases = pltpu.make_async_copy(phases_hbm, phases, load_sem.at[5])
    for load in (load_slots, load_momenta, load_per, load_eig, load_columns, load_phases):
        load.start()

    barrier = pltpu.get_barrier_semaphore()

    def greet(semaphore, peer, peer_time):
        pl.semaphore_signal(
            semaphore, inc=1, device_id={"space": peer, "tm": peer_time}, device_id_type=MESH
        )

    def greets(source, source_time, target, target_time):
        def hub(place, at):
            return (place >= n // 4) & (place < n // 4 + hubs) & (at == hub_time)

        step = target - source
        ahead = (step > 0) & (lax.rem(step + n, 2) == 0)
        pair = (lax.div(source, 2) == lax.div(target, 2)) & (step != 0)
        near = (source_time == target_time) & (ahead | pair)
        other = (step != 0) | (source_time != target_time)
        return other & (hub(source, source_time) | hub(target, target_time) | near)

    expected = 0
    for other in range(times):
        for peer in range(n):
            pl.when(greets(me, time, peer, other))(functools.partial(greet, barrier, peer, other))
            expected = expected + greets(peer, other, me, time).astype(jnp.int32)

    def remote(src, dst, recv, peer, peer_time=None):
        peer_time = time if peer_time is None else peer_time
        return pltpu.make_async_remote_copy(
            src_ref=src, dst_ref=dst, send_sem=send_sem.at[0], recv_sem=recv,
            device_id={"space": peer, "tm": peer_time}, device_id_type=MESH,
        )

    def arrived(ref, sem):
        pltpu.make_async_copy(ref, ref, sem).wait()

    def sink_of(owner):
        return sink.at[owner]

    late = line >= lines // 2
    toward = jnp.where(late, 1, -1)

    def enter():
        pl.semaphore_wait(barrier, expected)

        @pl.when(is_hub)
        def _():
            for other in range(times):
                greet(ready.at[0], me + 2 * toward, other)
                if other < times - 1:
                    greet(ready.at[0], me, other)

        for lower in range(lines - 1):
            pl.when(lower < line)(
                functools.partial(greet, reply.at[line], 2 * lower + side, time)
            )

    def send_up(target):
        pl.semaphore_wait(reply.at[target], 1)
        send_sink(target)

    def send_sink(target):
        remote(sink_of(me), sink_of(me), line_recv.at[line], 2 * target + side).start()

    def send_near():
        remote(sink_of(me), sink_of(me), near_recv.at[0], partner).start()

    load_momenta.wait()
    cosine, sine = site_phases(lambda i: momenta[0, i], me * sites, sites, extent_x, (sites, eig_count))
    waves[0] = cosine
    waves[1] = sine
    load_slots.wait()
    load_per.wait()
    sink[me] = per[slots[1]].reshape(8, rows, eig_count)

    early = late & (time == 0)

    @pl.when(early)
    def _():
        enter()
        send_sink(0)
        send_near()

    load_eig.wait()
    eig32[...] = eig[...].astype(F32)
    for color in range(3):
        real = eig32[pl.ds(2 * color, sites, stride=6), :]
        imag = eig32[pl.ds(2 * color + 1, sites, stride=6), :]
        wave_real = (waves[0] * real - waves[1] * imag).astype(BF16)
        wave_imag = (waves[1] * real + waves[0] * imag).astype(BF16)
        low = pl.ds(2 * color * sites, sites)
        high = pl.ds((2 * color + 1) * sites, sites)
        left[low, :] = real.astype(BF16)
        left[high, :] = imag.astype(BF16)
        right[low, :eig_count] = wave_real
        right[low, eig_count:] = wave_imag
        right[high, :eig_count] = wave_imag
        right[high, eig_count:] = -wave_real
    whole = lax.dot_general(
        left[...], right[...], (((0,), (0,)), ((), ())), preferred_element_type=F32
    )
    part[...] = whole.astype(part.dtype).reshape(hubs, hub_rows, 2 * eig_count)

    def send_red():
        for i in range(hubs):
            j = jnp.where(me < n // 2, hubs - 1 - i, i)
            copy = remote(
                part.at[j], sums.at[time * n + me], red_recv.at[0], j + n // 4, hub_time
            )
            pl.when((slot != j) | is_leaf)(copy.start)

    def send_turned():
        for k in range(1, n):
            peer = lax.rem(me + k, n)
            remote(turned.at[peer], picked.at[me], turn_recv.at[0], peer).start()

    pl.when(jnp.logical_not(early))(enter)
    send_red()

    @pl.when(jnp.logical_not(early))
    def _():
        send_near()
        pl.when(line > 0)(lambda: send_sink(0))

    first = per[slots[0]].reshape(8 * rows, eig_count).astype(F32)
    turned[...] = first.T.astype(BF16).reshape(n, rows, 8 * rows)
    picked[me] = turned[me]

    @pl.when(line < lines // 2)
    def _():
        pl.when(line == 0)(lambda: send_up(1))
        send_up(2)

    pl.when(is_leaf)(lambda: pl.semaphore_wait(ready.at[0], 1))
    send_turned()
    pl.when(line < lines - 1)(lambda: send_up(lines - 1))
    pl.when(late)(lambda: send_sink(1))
    pl.when(line == lines - 1)(lambda: send_sink(2))

    def forward(origin):
        owner = 2 * origin + side
        arrived(sink.at[owner], line_recv.at[origin])
        return owner

    def pass_on(origin):
        owner = forward(origin)
        remote(sink.at[owner], sink.at[owner], near_recv.at[0], partner).start()

    @pl.when(is_hub)
    def _():
        arrived(sums.at[pl.ds(0, times * n - 1)], red_recv.at[0])
        for other in range(times):
            own = other == times - 1
            total = part[here].astype(F32) if own else sums[other * n + me].astype(F32)
            for k in range(1, n):
                total = total + sums[other * n + lax.rem(me + k, n)].astype(F32)
            source = mfull.at[here] if own else spread.at[other]
            source[...] = total.astype(BF16)
            for k in range(n - own):
                peer = k + (k >= me).astype(jnp.int32) if own else k
                remote(source, mfull.at[here], all_recv.at[0], peer, other).start()

    @pl.when((line > 0) & (line < lines - 1))
    def _():
        pass_on(jnp.where(late, 1, 0))
        pass_on(jnp.where(late, 0, 2))
        pass_on(lines - 1)

    @pl.when((line == 0) | (line == lines - 1))
    def _():
        for k in range(1, lines):
            pass_on(line - k * toward)

    arrived(picked.at[pl.ds(0, n - 1)], turn_recv.at[0])
    group = lax.broadcasted_iota(jnp.int32, (rows, eig_count), 1) // rows
    chunks = [None] * 8
    for k in range(n):
        block = picked[k].astype(F32)
        for c in range(8):
            turn = (k - c) % 8
            moved = pltpu.roll(block, turn * rows, 1) if turn else block
            chunks[c] = moved if chunks[c] is None else jnp.where(group == k, moved, chunks[c])
    sources = jnp.concatenate(chunks[0::2] + chunks[1::2], axis=0).astype(BF16)
    load_columns.wait()
    load_phases.wait()
    arrived(sink.at[pl.ds(0, lines)], near_recv.at[0])

    @pl.when(is_hub)
    def _():
        arrived(mfull.at[pl.ds(0, hubs - 1)], all_recv.at[0])

    @pl.when(is_leaf)
    def _():
        arrived(mfull, all_recv.at[0])

    half = 4 * rows
    both = jnp.dot(sources, mfull[...].reshape(eig_count, 2 * eig_count), preferred_element_type=F32)
    cross_real = ((both[:half, :eig_count] + both[half:, eig_count:]) * factor).astype(BF16)
    cross_imag = ((both[:half, eig_count:] - both[half:, :eig_count]) * factor).astype(BF16)
    stacked = jnp.concatenate(
        [
            jnp.concatenate([cross_real, -cross_imag], axis=1),
            jnp.concatenate([cross_imag, cross_real], axis=1),
        ],
        axis=0,
    )
    for pair in range(2):
        table = jnp.concatenate(
            [
                jnp.concatenate(
                    [sink[owner, 4 * pair + 2 * i + c] for c in range(2) for owner in range(n)], axis=0
                )
                for i in range(2)
            ],
            axis=1,
        )
        result = jnp.dot(stacked, table, preferred_element_type=F32)
        for i in range(2):
            for part_of in range(2):
                for spin in range(4):
                    base = (part_of * 4 + spin) * rows
                    blocks[part_of, spin * 4 + 2 * pair + i] = result[
                        base : base + rows, i * eig_count : (i + 1) * eig_count
                    ]
    for g in range(gammas):
        real = imag = None
        for spin in range(4):
            phase = phases[spin, g]
            odd = phase % 2
            index = spin * 4 + columns[spin, g]
            sign_real = jnp.where((phase == 0) | (phase == 3), 1.0, -1.0).astype(F32)
            sign_imag = jnp.where(phase < 2, 1.0, -1.0).astype(F32)
            term_real = sign_real * blocks[odd, index]
            term_imag = sign_imag * blocks[1 - odd, index]
            real = term_real if real is None else real + term_real
            imag = term_imag if imag is None else imag + term_imag
        out_ref[pl.ds(2 * g, rows, stride=2 * gammas), :] = real
        out_ref[pl.ds(2 * g + 1, rows, stride=2 * gammas), :] = imag

    unit = 4 * rows
    plain = hubs * unit + 2 * lines * 8 * rows + (n - 1) * rows - 8 * rows
    extra = (times * n - 2) * unit

    @pl.when(is_hub)
    def _():
        arrived(volume.at[pl.ds(0, plain + extra)], send_sem.at[0])

    @pl.when(is_leaf)
    def _():
        arrived(volume.at[pl.ds(0, plain)], send_sem.at[0])


def store_kernel(source, target, sem):
    copy = pltpu.make_async_copy(source, target, sem.at[0])
    copy.start()
    copy.wait()


def on_device_kernel(eigvecs, perambulator, momenta, source_slots, gamma_columns, gamma_phases):
    sites, eig_count = eigvecs.shape[1], eigvecs.shape[4]
    n = lax.axis_size("space")
    times = lax.axis_size("tm")
    rows = eig_count // n
    total_sites = sites * n
    gammas = gamma_columns.shape[0]
    stored = perambulator.shape[1]
    body = functools.partial(
        kernel, n, sites, total_sites // (LY * LZ), 1.0 / math.sqrt(12.0 * total_sites)
    )
    dma = pltpu.SemaphoreType.DMA
    hbm = pl.BlockSpec(memory_space=pltpu.HBM)
    out = pl.pallas_call(
        body,
        out_shape=pltpu.VMEM((rows * gammas * 2, eig_count), F32),
        in_specs=[hbm] * 6,
        out_specs=pl.BlockSpec(memory_space=pltpu.VMEM),
        scratch_shapes=[
            pltpu.SMEM(momenta.shape, jnp.int32),
            pltpu.SMEM(source_slots.shape, jnp.int32),
            pltpu.SMEM((4, gammas), jnp.int32),
            pltpu.SMEM((4, gammas), jnp.int32),
            pltpu.VMEM((sites * 6, eig_count), BF16),
            pltpu.VMEM((sites * 6, eig_count), F32),
            pltpu.VMEM((2, sites, eig_count), F32),
            pltpu.VMEM((sites * 6, eig_count), BF16),
            pltpu.VMEM((sites * 6, 2 * eig_count), BF16),
            pltpu.VMEM((stored, 4, 2, rows, eig_count), BF16),
            pltpu.VMEM((n, 8, rows, eig_count), BF16),
            pltpu.VMEM((n, rows, 8 * rows), BF16),
            pltpu.VMEM((n, rows, 8 * rows), BF16),
            pltpu.VMEM((n // 2, 2 * rows, 2 * eig_count), WIRE),
            pltpu.VMEM((times * n, 2 * rows, 2 * eig_count), WIRE),
            pltpu.VMEM((times - 1, 2 * rows, 2 * eig_count), BF16),
            pltpu.VMEM((n // 2, 2 * rows, 2 * eig_count), BF16),
            pltpu.VMEM((2, 16, rows, eig_count), F32),
            pltpu.VMEM((24 * eig_count, eig_count), BF16),
            pltpu.SemaphoreType.REGULAR((1,)),
            pltpu.SemaphoreType.REGULAR((n // 2,)),
            dma((6,)),
            dma((1,)),
            dma((1,)),
            dma((1,)),
            dma((1,)),
            dma((1,)),
            dma((n // 2,)),
        ],
        compiler_params=pltpu.CompilerParams(
            collective_id=0, has_side_effects=True, vmem_limit_bytes=VMEM_LIMIT
        ),
    )(
        *(
            pltpu.with_memory_space_constraint(array, pltpu.HBM)
            for array in (
                momenta,
                source_slots,
                gamma_columns.T,
                gamma_phases.T,
                eigvecs.reshape(sites * 6, eig_count),
                perambulator[0],
            )
        )
    )
    done = pl.pallas_call(
        store_kernel,
        out_shape=jax.ShapeDtypeStruct(out.shape, F32),
        in_specs=[pl.BlockSpec(memory_space=pl.ANY)],
        out_specs=hbm,
        scratch_shapes=[dma((1,))],
        compiler_params=pltpu.CompilerParams(vmem_limit_bytes=VMEM_LIMIT),
    )(out)
    return done.reshape(1, rows, 1, gammas, 2, eig_count)


def on_device_plain(eigvecs, perambulator, momenta, source_slots, gamma_columns, gamma_phases):
    sites, eig_count = eigvecs.shape[1], eigvecs.shape[4]
    n = lax.axis_size("space")
    total_sites = sites * n
    extent_x = total_sites // (LY * LZ)
    factor = 1.0 / math.sqrt(12.0 * total_sites)
    first_site = lax.axis_index("space") * sites
    chosen = jnp.take(perambulator[0], source_slots, axis=0)
    sinks = lax.all_gather(chosen[1], "space", axis=2, tiled=True)
    turned = lax.all_to_all(chosen[0], "space", split_axis=3, concat_axis=2, tiled=True)
    real = eigvecs[0, :, :, 0].astype(F32)
    imag = eigvecs[0, :, :, 1].astype(F32)
    flat = eigvecs[0].reshape(sites * 6, eig_count)
    tables = []
    for p in range(momenta.shape[0]):
        cosine, sine = site_phases(
            lambda i, p=p: momenta[p, i], first_site, sites, extent_x, (sites, 1, 1)
        )
        wave_real = cosine * real - sine * imag
        wave_imag = sine * real + cosine * imag
        upper = jnp.concatenate([wave_real, wave_imag], axis=2)
        lower = jnp.concatenate([wave_imag, -wave_real], axis=2)
        waves = jnp.stack([upper, lower], axis=2).astype(BF16).reshape(sites * 6, 2 * eig_count)
        tables.append(
            lax.dot_general(flat, waves, (((0,), (0,)), ((), ())), preferred_element_type=F32)
        )
    whole = lax.psum(jnp.stack(tables), "space").astype(BF16)
    turned_whole = jnp.concatenate([whole[:, :, eig_count:], -whole[:, :, :eig_count]], axis=2)
    both = jnp.stack([whole, turned_whole], axis=1)
    cross = jnp.einsum("skla,pklm->aspm", turned, both, preferred_element_type=F32)
    cross_real, cross_imag = cross[..., :eig_count], cross[..., eig_count:]
    stacked = jnp.stack(
        [
            jnp.stack([cross_real, -cross_imag], axis=-2),
            jnp.stack([cross_imag, cross_real], axis=-2),
        ],
        axis=3,
    ).astype(BF16)
    blocks = jnp.einsum("asphkl,tklb->apsthb", stacked, sinks, preferred_element_type=F32)
    spins = jnp.arange(4, dtype=jnp.int32)
    matches = (gamma_columns[:, :, None] == spins).astype(F32)
    real_sign = (gamma_phases == 0).astype(F32) - (gamma_phases == 2).astype(F32)
    imag_sign = (gamma_phases == 1).astype(F32) - (gamma_phases == 3).astype(F32)
    mix_real = matches * real_sign[:, :, None]
    mix_imag = matches * imag_sign[:, :, None]
    mix = jnp.stack(
        [jnp.stack([mix_real, -mix_imag], axis=-1), jnp.stack([mix_imag, mix_real], axis=-1)],
        axis=1,
    )
    meson = factor * jnp.einsum("gosth,apsthb->apgob", mix, blocks, precision=lax.Precision.HIGHEST)
    return meson[None]


def on_device(eigvecs, perambulator, momenta, *rest):
    n = lax.axis_size("space")
    rows = perambulator.shape[4]
    small = eigvecs.shape[1] % 16 == 0 and eigvecs.shape[4] == 128
    if rows == 16 and n == 8 and lax.axis_size("tm") == 2 and momenta.shape[0] == 1 and small:
        return on_device_kernel(eigvecs, perambulator, momenta, *rest)
    return on_device_plain(eigvecs, perambulator, momenta, *rest)


def solution(mesh):
    in_specs = (
        P(("cfg", "tm"), "space", None, None, None),
        P(("cfg", "tm"), None, None, None, "space", None),
        P(),
        P(),
        P(),
        P(),
    )
    out_specs = P(("cfg", "tm"), "space", None, None, None, None)
    return jax.shard_map(
        on_device, mesh=mesh, in_specs=in_specs, out_specs=out_specs, check_vma=False
    )
```

```python
import functools
import math

import jax
import jax.numpy as jnp
from jax import lax
from jax.experimental import pallas as pl
from jax.experimental.pallas import tpu as pltpu
from jax.sharding import PartitionSpec as P

LY = 48
LZ = 48
WIRE = jnp.bfloat16
F32 = jnp.float32
BF16 = jnp.bfloat16
MESH = pl.DeviceIdType.MESH
VMEM_LIMIT = 32 * 1024 * 1024


def site_phases(momenta_at, first_site, site_count, extent_x, shape):
    site = (lax.broadcasted_iota(jnp.int32, shape, 0) + first_site).astype(F32)
    lines = jnp.floor((site + 0.5) * (1.0 / LZ))
    coord_x = jnp.floor((lines + 0.5) * (1.0 / LY))
    coord_y = lines - LY * coord_x
    coord_z = site - LZ * lines

    def share(momentum, coord, extent):
        turn = momentum.astype(F32) * coord * (1.0 / extent)
        return turn - jnp.floor(turn)

    turns = (
        share(momenta_at(0), coord_x, extent_x)
        + share(momenta_at(1), coord_y, LY)
        + share(momenta_at(2), coord_z, LZ)
    )
    turns = turns - jnp.floor(turns + 0.5)
    half = math.pi * turns
    square = half * half
    sine = jnp.full(shape, 1.0 / 6227020800.0, F32)
    for term in (-1.0 / 39916800.0, 1.0 / 362880.0, -1.0 / 5040.0, 1.0 / 120.0, -1.0 / 6.0, 1.0):
        sine = sine * square + term
    sine = sine * half
    cosine = jnp.full(shape, 1.0 / 479001600.0, F32)
    for term in (-1.0 / 3628800.0, 1.0 / 40320.0, -1.0 / 720.0, 1.0 / 24.0, -0.5, 1.0):
        cosine = cosine * square + term
    return 1.0 - 2.0 * sine * sine, 2.0 * sine * cosine


def kernel(
    n, sites, extent_x, factor,
    momenta_hbm, slots_hbm, columns_hbm, phases_hbm, eig_hbm, per_hbm, out_ref,
    momenta, slots, columns, phases, picks, eig, eig32, waves, left, right, per, sink, turned, picked,
    part, sums, spread, mfull, blocks, volume,
    ready, reply, load_sem, send_sem, red_recv, all_recv, turn_recv, near_recv, line_recv,
):
    me = lax.axis_index("space")
    time = lax.axis_index("tm")
    times = lax.axis_size("tm")
    hub_time = times - 1
    eig_count = eig.shape[1]
    rows = eig_count // n
    gammas = columns.shape[1]
    hubs = n // 2
    hub_rows = eig_count // hubs
    slot = me - n // 4
    inner = (slot >= 0) & (slot < hubs)
    is_hub = inner & (time == hub_time)
    is_leaf = jnp.logical_not(is_hub)
    here = jnp.clip(slot, 0, hubs - 1)
    side = lax.rem(me, 2)
    line = lax.div(me, 2)
    lines = n // 2
    partner = me + 1 - 2 * side

    load_per = pltpu.make_async_copy(per_hbm, per, load_sem.at[0])
    load_eig = pltpu.make_async_copy(eig_hbm, eig, load_sem.at[1])
    load_slots = pltpu.make_async_copy(slots_hbm, slots, load_sem.at[2])
    load_momenta = pltpu.make_async_copy(momenta_hbm, momenta, load_sem.at[3])
    load_columns = pltpu.make_async_copy(columns_hbm, columns, load_sem.at[4])
    load_phases = pltpu.make_async_copy(phases_hbm, phases, load_sem.at[5])
    for load in (load_slots, load_momenta, load_per, load_eig, load_columns, load_phases):
        load.start()

    barrier = pltpu.get_barrier_semaphore()

    def greet(semaphore, peer, peer_time):
        pl.semaphore_signal(
            semaphore, inc=1, device_id={"space": peer, "tm": peer_time}, device_id_type=MESH
        )

    for j in range(hubs):
        peer = j + n // 4
        pl.when((me != peer) | is_leaf)(functools.partial(greet, barrier, peer, hub_time))
    for other in range(times):
        for peer in list(range(n // 4)) + list(reversed(range(n // 4, n))):
            if n // 4 <= peer < n // 4 + hubs and other == times - 1:
                continue
            across = (line == peer // 2) & (side != peer % 2)
            above = (side == peer % 2) & (line < peer // 2)
            pl.when(is_hub | ((time == other) & (across | above)))(
                functools.partial(greet, barrier, peer, other)
            )
    lower = jnp.where(time == hub_time, (line == lines - 1).astype(jnp.int32), line)
    expected = jnp.where(is_hub, times * n - 1, hubs + 1 + lower)

    def remote(src, dst, recv, peer, peer_time=None):
        peer_time = time if peer_time is None else peer_time
        return pltpu.make_async_remote_copy(
            src_ref=src, dst_ref=dst, send_sem=send_sem.at[0], recv_sem=recv,
            device_id={"space": peer, "tm": peer_time}, device_id_type=MESH,
        )

    def arrived(ref, sem):
        pltpu.make_async_copy(ref, ref, sem).wait()

    def sink_of(owner):
        return sink.at[owner]

    late = line >= lines // 2
    toward = jnp.where(late, 1, -1)

    def enter():
        pl.semaphore_wait(barrier, expected)

        @pl.when(is_hub)
        def _():
            for other in range(times):
                greet(ready.at[0], me + 2 * toward, other)
                if other < times - 1:
                    greet(ready.at[0], me, other)

        for lower in range(lines - 1):
            pl.when((lower < line) & ((lower != 1) | (line < lines - 1)))(
                functools.partial(greet, reply.at[line], 2 * lower + side, time)
            )

    def send_up(target):
        pl.semaphore_wait(reply.at[target], 1)
        send_sink(target)

    def send_sink(target):
        remote(sink_of(me), sink_of(me), line_recv.at[line], 2 * target + side).start()

    def send_near():
        remote(sink_of(me), sink_of(me), near_recv.at[0], partner).start()

    load_momenta.wait()
    cosine, sine = site_phases(lambda i: momenta[0, i], me * sites, sites, extent_x, (sites, eig_count))
    waves[0] = cosine
    waves[1] = sine
    load_slots.wait()
    load_per.wait()
    sink[me] = per[slots[1]].reshape(8, rows, eig_count)

    early = late & (time == 0)

    @pl.when(early)
    def _():
        enter()
        send_sink(jnp.where(line == lines - 1, 0, 1))
        send_near()

    load_eig.wait()
    eig32[...] = eig[...].astype(F32)
    for color in range(3):
        real = eig32[pl.ds(2 * color, sites, stride=6), :]
        imag = eig32[pl.ds(2 * color + 1, sites, stride=6), :]
        wave_real = (waves[0] * real - waves[1] * imag).astype(BF16)
        wave_imag = (waves[1] * real + waves[0] * imag).astype(BF16)
        span = pl.ds(color * sites, sites)
        left[span, :eig_count] = real.astype(BF16)
        left[span, eig_count:] = imag.astype(BF16)
        right[span, :eig_count] = wave_real
        right[span, eig_count:] = wave_imag
    whole = lax.dot_general(
        left[...], right[...], (((0,), (0,)), ((), ())), preferred_element_type=F32
    )
    whole = jnp.concatenate(
        [
            whole[:eig_count, :eig_count] + whole[eig_count:, eig_count:],
            whole[:eig_count, eig_count:] - whole[eig_count:, :eig_count],
        ],
        axis=1,
    )
    part[...] = whole.astype(part.dtype).reshape(hubs, hub_rows, 2 * eig_count)

    def send_red():
        for i in range(hubs):
            j = 2 * (i // 2) + (1 - i % 2) * (1 - 2 * side) + side
            j = jnp.where(me < n // 2, (j + 2) % 4, j)
            copy = remote(
                part.at[j], sums.at[time * n + me], red_recv.at[0], j + n // 4, hub_time
            )
            pl.when((slot != j) | is_leaf)(copy.start)

    def send_turned():
        for k in range(1, n):
            peer = lax.rem(me + k, n)
            remote(turned.at[peer], picked.at[me], turn_recv.at[0], peer).start()

    pl.when(jnp.logical_not(early))(enter)
    send_red()

    @pl.when(jnp.logical_not(early))
    def _():
        send_near()
        pl.when((line == 1) | (line == lines - 1))(lambda: send_sink(0))
        pl.when(line == lines - 2)(lambda: send_sink(0))
        pl.when(line == lines - 2)(lambda: send_sink(1))

    first = per[slots[0]].reshape(8 * rows, eig_count).astype(F32)
    turned[...] = first.T.astype(BF16).reshape(n, rows, 8 * rows)
    picked[me] = turned[me]

    @pl.when(line < lines // 2)
    def _():
        pl.when(line == 0)(lambda: send_up(1))
        send_up(2)

    pl.when(is_leaf)(lambda: pl.semaphore_wait(ready.at[0], 1))
    send_turned()
    pl.when((line == 0) | (line == lines - 2))(lambda: send_up(lines - 1))
    pl.when(line == lines - 1)(lambda: send_sink(1))
    pl.when(line == lines - 1)(lambda: send_sink(2))

    def forward(origin):
        owner = 2 * origin + side
        arrived(sink.at[owner], line_recv.at[origin])
        return owner

    def pass_on(origin):
        owner = forward(origin)
        remote(sink.at[owner], sink.at[owner], near_recv.at[0], partner).start()

    inner_line = (line > 0) & (line < lines - 1)

    @pl.when(is_hub)
    def _():
        arrived(sums.at[pl.ds(0, times * n - 1)], red_recv.at[0])
        for other in range(times):
            own = other == times - 1
            total = part[here].astype(F32) if own else sums[other * n + me].astype(F32)
            for k in range(1, n):
                total = total + sums[other * n + lax.rem(me + k, n)].astype(F32)
            source = mfull.at[here] if own else spread.at[other]
            source[...] = total.astype(BF16)
            for k in range(n - own):
                peer = k + (k >= me).astype(jnp.int32) if own else k
                remote(source, mfull.at[here], all_recv.at[0], peer, other).start()

    relays = inner_line & (late | (time == 0))

    @pl.when(inner_line & jnp.logical_not(relays))
    def _():
        pass_on(line - toward)

    @pl.when(relays)
    def _():
        origin = line - toward
        owner = forward(origin)
        ends = me + 2 * toward
        block = sink.at[owner]
        remote(block, block, line_recv.at[line + toward], ends + 1 - 2 * side).start()
        remote(block, block, line_recv.at[origin], ends).start()
        remote(block, block, near_recv.at[0], partner).start()

    @pl.when(inner_line)
    def _():
        pass_on(line + toward)
        pass_on(line - 2 * toward)

    plain_end = (line == 0) & (time == hub_time)

    @pl.when(jnp.logical_not(inner_line))
    def _():
        pass_on(line - toward)
        pl.when(plain_end)(lambda: pass_on(line - 2 * toward))
        pass_on(line - 3 * toward)

    arrived(picked.at[pl.ds(0, n - 1)], turn_recv.at[0])
    group = lax.broadcasted_iota(jnp.int32, (rows, eig_count), 1) // rows
    chunks = [None] * 8
    for k in range(n):
        block = picked[k].astype(F32)
        for c in range(8):
            turn = (k - c) % 8
            moved = pltpu.roll(block, turn * rows, 1) if turn else block
            chunks[c] = moved if chunks[c] is None else jnp.where(group == k, moved, chunks[c])
    sources = jnp.concatenate(chunks[0::2] + chunks[1::2], axis=0).astype(BF16)
    load_columns.wait()
    load_phases.wait()
    for g in range(gammas):
        for spin in range(4):
            phase = phases[spin, g]
            place = spin * 4 + columns[spin, g]
            picks[0, 4 * g + spin] = phase * 16 + place
            picks[1, 4 * g + spin] = lax.rem(phase + 3, 4) * 16 + place

    @pl.when(inner_line | plain_end)
    def _():
        arrived(sink.at[pl.ds(0, lines)], near_recv.at[0])

    @pl.when(jnp.logical_not(inner_line | plain_end))
    def _():
        forward(line - 2 * toward)
        arrived(sink.at[me], line_recv.at[line])
        arrived(sink.at[pl.ds(0, lines - 1)], near_recv.at[0])

    @pl.when(is_hub)
    def _():
        arrived(mfull.at[pl.ds(0, hubs - 1)], all_recv.at[0])

    @pl.when(is_leaf)
    def _():
        arrived(mfull, all_recv.at[0])

    half = 4 * rows
    both = jnp.dot(sources, mfull[...].reshape(eig_count, 2 * eig_count), preferred_element_type=F32)
    cross_real = ((both[:half, :eig_count] + both[half:, eig_count:]) * factor).astype(BF16)
    cross_imag = ((both[:half, eig_count:] - both[half:, :eig_count]) * factor).astype(BF16)
    stacked = jnp.concatenate(
        [
            jnp.concatenate([cross_real, -cross_imag], axis=1),
            jnp.concatenate([cross_imag, cross_real], axis=1),
        ],
        axis=0,
    )
    for pair in range(2):
        table = jnp.concatenate(
            [
                jnp.concatenate(
                    [sink[owner, 4 * pair + 2 * i + c] for c in range(2) for owner in range(n)], axis=0
                )
                for i in range(2)
            ],
            axis=1,
        )
        result = jnp.dot(stacked, table, preferred_element_type=F32)
        for i in range(2):
            for spin in range(4):
                place = spin * 4 + 2 * pair + i
                columns_of = slice(i * eig_count, (i + 1) * eig_count)
                real = result[spin * rows : (spin + 1) * rows, columns_of]
                imag = result[(4 + spin) * rows : (5 + spin) * rows, columns_of]
                for turn, block in enumerate((real, -imag, -real, imag)):
                    blocks[turn * 16 + place] = block
    for g in range(gammas):
        for which in range(2):
            term = blocks[picks[which, 4 * g]]
            for spin in range(1, 4):
                term = term + blocks[picks[which, 4 * g + spin]]
            out_ref[pl.ds(2 * g + which, rows, stride=2 * gammas), :] = term

    unit = 4 * rows
    plain = hubs * unit + 2 * lines * 8 * rows + (n - 1) * rows - 8 * rows
    extra = (times * n - 2) * unit

    block = 8 * rows
    direct = time == hub_time
    changes = (
        (inner_line & (late | jnp.logical_not(direct)) & jnp.logical_not(late & direct), block),
        (late & inner_line & direct, 2 * block),
        (jnp.logical_not(late) & inner_line & direct, -block),
        (plain_end, 0),
        (jnp.logical_not(inner_line | plain_end), -block),
    )
    for hub, spreading in ((is_hub, extra), (is_leaf, 0)):
        for some, change in changes:
            pl.when(hub & some)(
                functools.partial(
                    arrived, volume.at[pl.ds(0, plain + spreading + change)], send_sem.at[0]
                )
            )


def store_kernel(source, target, sem):
    copy = pltpu.make_async_copy(source, target, sem.at[0])
    copy.start()
    copy.wait()


def on_device_kernel(eigvecs, perambulator, momenta, source_slots, gamma_columns, gamma_phases):
    sites, eig_count = eigvecs.shape[1], eigvecs.shape[4]
    n = lax.axis_size("space")
    times = lax.axis_size("tm")
    rows = eig_count // n
    total_sites = sites * n
    gammas = gamma_columns.shape[0]
    stored = perambulator.shape[1]
    body = functools.partial(
        kernel, n, sites, total_sites // (LY * LZ), 1.0 / math.sqrt(12.0 * total_sites)
    )
    dma = pltpu.SemaphoreType.DMA
    hbm = pl.BlockSpec(memory_space=pltpu.HBM)
    out = pl.pallas_call(
        body,
        out_shape=pltpu.VMEM((rows * gammas * 2, eig_count), F32),
        in_specs=[hbm] * 6,
        out_specs=pl.BlockSpec(memory_space=pltpu.VMEM),
        scratch_shapes=[
            pltpu.SMEM(momenta.shape, jnp.int32),
            pltpu.SMEM(source_slots.shape, jnp.int32),
            pltpu.SMEM((4, gammas), jnp.int32),
            pltpu.SMEM((4, gammas), jnp.int32),
            pltpu.SMEM((2, 4 * gammas), jnp.int32),
            pltpu.VMEM((sites * 6, eig_count), BF16),
            pltpu.VMEM((sites * 6, eig_count), F32),
            pltpu.VMEM((2, sites, eig_count), F32),
            pltpu.VMEM((sites * 3, 2 * eig_count), BF16),
            pltpu.VMEM((sites * 3, 2 * eig_count), BF16),
            pltpu.VMEM((stored, 4, 2, rows, eig_count), BF16),
            pltpu.VMEM((n, 8, rows, eig_count), BF16),
            pltpu.VMEM((n, rows, 8 * rows), BF16),
            pltpu.VMEM((n, rows, 8 * rows), BF16),
            pltpu.VMEM((n // 2, 2 * rows, 2 * eig_count), WIRE),
            pltpu.VMEM((times * n, 2 * rows, 2 * eig_count), WIRE),
            pltpu.VMEM((times - 1, 2 * rows, 2 * eig_count), BF16),
            pltpu.VMEM((n // 2, 2 * rows, 2 * eig_count), BF16),
            pltpu.VMEM((64, rows, eig_count), F32),
            pltpu.VMEM((24 * eig_count, eig_count), BF16),
            pltpu.SemaphoreType.REGULAR((1,)),
            pltpu.SemaphoreType.REGULAR((n // 2,)),
            dma((6,)),
            dma((1,)),
            dma((1,)),
            dma((1,)),
            dma((1,)),
            dma((1,)),
            dma((n // 2,)),
        ],
        compiler_params=pltpu.CompilerParams(
            collective_id=0, has_side_effects=True, vmem_limit_bytes=VMEM_LIMIT
        ),
    )(
        *(
            pltpu.with_memory_space_constraint(array, pltpu.HBM)
            for array in (
                momenta,
                source_slots,
                gamma_columns.T,
                gamma_phases.T,
                eigvecs.reshape(sites * 6, eig_count),
                perambulator[0],
            )
        )
    )
    done = pl.pallas_call(
        store_kernel,
        out_shape=jax.ShapeDtypeStruct(out.shape, F32),
        in_specs=[pl.BlockSpec(memory_space=pl.ANY)],
        out_specs=hbm,
        scratch_shapes=[dma((1,))],
        compiler_params=pltpu.CompilerParams(vmem_limit_bytes=VMEM_LIMIT),
    )(out)
    return done.reshape(1, rows, 1, gammas, 2, eig_count)


def on_device_plain(eigvecs, perambulator, momenta, source_slots, gamma_columns, gamma_phases):
    sites, eig_count = eigvecs.shape[1], eigvecs.shape[4]
    n = lax.axis_size("space")
    total_sites = sites * n
    extent_x = total_sites // (LY * LZ)
    factor = 1.0 / math.sqrt(12.0 * total_sites)
    first_site = lax.axis_index("space") * sites
    chosen = jnp.take(perambulator[0], source_slots, axis=0)
    sinks = lax.all_gather(chosen[1], "space", axis=2, tiled=True)
    turned = lax.all_to_all(chosen[0], "space", split_axis=3, concat_axis=2, tiled=True)
    real = eigvecs[0, :, :, 0].astype(F32)
    imag = eigvecs[0, :, :, 1].astype(F32)
    flat = eigvecs[0].reshape(sites * 6, eig_count)
    tables = []
    for p in range(momenta.shape[0]):
        cosine, sine = site_phases(
            lambda i, p=p: momenta[p, i], first_site, sites, extent_x, (sites, 1, 1)
        )
        wave_real = cosine * real - sine * imag
        wave_imag = sine * real + cosine * imag
        upper = jnp.concatenate([wave_real, wave_imag], axis=2)
        lower = jnp.concatenate([wave_imag, -wave_real], axis=2)
        waves = jnp.stack([upper, lower], axis=2).astype(BF16).reshape(sites * 6, 2 * eig_count)
        tables.append(
            lax.dot_general(flat, waves, (((0,), (0,)), ((), ())), preferred_element_type=F32)
        )
    whole = lax.psum(jnp.stack(tables), "space").astype(BF16)
    turned_whole = jnp.concatenate([whole[:, :, eig_count:], -whole[:, :, :eig_count]], axis=2)
    both = jnp.stack([whole, turned_whole], axis=1)
    cross = jnp.einsum("skla,pklm->aspm", turned, both, preferred_element_type=F32)
    cross_real, cross_imag = cross[..., :eig_count], cross[..., eig_count:]
    stacked = jnp.stack(
        [
            jnp.stack([cross_real, -cross_imag], axis=-2),
            jnp.stack([cross_imag, cross_real], axis=-2),
        ],
        axis=3,
    ).astype(BF16)
    blocks = jnp.einsum("asphkl,tklb->apsthb", stacked, sinks, preferred_element_type=F32)
    spins = jnp.arange(4, dtype=jnp.int32)
    matches = (gamma_columns[:, :, None] == spins).astype(F32)
    real_sign = (gamma_phases == 0).astype(F32) - (gamma_phases == 2).astype(F32)
    imag_sign = (gamma_phases == 1).astype(F32) - (gamma_phases == 3).astype(F32)
    mix_real = matches * real_sign[:, :, None]
    mix_imag = matches * imag_sign[:, :, None]
    mix = jnp.stack(
        [jnp.stack([mix_real, -mix_imag], axis=-1), jnp.stack([mix_imag, mix_real], axis=-1)],
        axis=1,
    )
    meson = factor * jnp.einsum("gosth,apsthb->apgob", mix, blocks, precision=lax.Precision.HIGHEST)
    return meson[None]


def on_device(eigvecs, perambulator, momenta, *rest):
    n = lax.axis_size("space")
    rows = perambulator.shape[4]
    small = eigvecs.shape[1] % 16 == 0 and eigvecs.shape[4] == 128
    if rows == 16 and n == 8 and lax.axis_size("tm") == 2 and momenta.shape[0] == 1 and small:
        return on_device_kernel(eigvecs, perambulator, momenta, *rest)
    return on_device_plain(eigvecs, perambulator, momenta, *rest)


def solution(mesh):
    in_specs = (
        P(("cfg", "tm"), "space", None, None, None),
        P(("cfg", "tm"), None, None, None, "space", None),
        P(),
        P(),
        P(),
        P(),
    )
    out_specs = P(("cfg", "tm"), "space", None, None, None, None)
    return jax.shard_map(
        on_device, mesh=mesh, in_specs=in_specs, out_specs=out_specs, check_vma=False
    )
```

```python
import functools
import math

import jax
import jax.numpy as jnp
from jax import lax
from jax.experimental import pallas as pl
from jax.experimental.pallas import tpu as pltpu
from jax.sharding import PartitionSpec as P

LY = 48
LZ = 48
WIRE = jnp.bfloat16
F32 = jnp.float32
BF16 = jnp.bfloat16
MESH = pl.DeviceIdType.MESH
VMEM_LIMIT = 32 * 1024 * 1024


def site_phases(momenta_at, first_site, site_count, extent_x, shape):
    site = (lax.broadcasted_iota(jnp.int32, shape, 0) + first_site).astype(F32)
    lines = jnp.floor((site + 0.5) * (1.0 / LZ))
    coord_x = jnp.floor((lines + 0.5) * (1.0 / LY))
    coord_y = lines - LY * coord_x
    coord_z = site - LZ * lines

    def share(momentum, coord, extent):
        turn = momentum.astype(F32) * coord * (1.0 / extent)
        return turn - jnp.floor(turn)

    turns = (
        share(momenta_at(0), coord_x, extent_x)
        + share(momenta_at(1), coord_y, LY)
        + share(momenta_at(2), coord_z, LZ)
    )
    turns = turns - jnp.floor(turns + 0.5)
    half = math.pi * turns
    square = half * half
    sine = jnp.full(shape, 1.0 / 6227020800.0, F32)
    for term in (-1.0 / 39916800.0, 1.0 / 362880.0, -1.0 / 5040.0, 1.0 / 120.0, -1.0 / 6.0, 1.0):
        sine = sine * square + term
    sine = sine * half
    cosine = jnp.full(shape, 1.0 / 479001600.0, F32)
    for term in (-1.0 / 3628800.0, 1.0 / 40320.0, -1.0 / 720.0, 1.0 / 24.0, -0.5, 1.0):
        cosine = cosine * square + term
    return 1.0 - 2.0 * sine * sine, 2.0 * sine * cosine


def kernel(
    n, sites, extent_x, factor,
    momenta_hbm, slots_hbm, columns_hbm, phases_hbm, eig_hbm, per_hbm, out_ref,
    momenta, slots, columns, phases, picks, eig, eig32, waves, left, right, per, sink, turned, picked,
    part, sums, spread, mfull, blocks, volume,
    ready, reply, load_sem, send_sem, red_recv, all_recv, turn_recv, near_recv, line_recv,
):
    me = lax.axis_index("space")
    time = lax.axis_index("tm")
    times = lax.axis_size("tm")
    hub_time = times - 1
    eig_count = eig.shape[1]
    rows = eig_count // n
    gammas = columns.shape[1]
    hubs = n // 2
    hub_rows = eig_count // hubs
    slot = me - n // 4
    inner = (slot >= 0) & (slot < hubs)
    is_hub = inner & (time == hub_time)
    is_leaf = jnp.logical_not(is_hub)
    here = jnp.clip(slot, 0, hubs - 1)
    side = lax.rem(me, 2)
    line = lax.div(me, 2)
    lines = n // 2
    partner = me + 1 - 2 * side

    load_per = pltpu.make_async_copy(per_hbm, per, load_sem.at[0])
    load_eig = pltpu.make_async_copy(eig_hbm, eig, load_sem.at[1])
    load_slots = pltpu.make_async_copy(slots_hbm, slots, load_sem.at[2])
    load_momenta = pltpu.make_async_copy(momenta_hbm, momenta, load_sem.at[3])
    load_columns = pltpu.make_async_copy(columns_hbm, columns, load_sem.at[2])
    load_phases = pltpu.make_async_copy(phases_hbm, phases, load_sem.at[3])
    for load in (load_slots, load_momenta, load_per, load_eig):
        load.start()

    barrier = pltpu.get_barrier_semaphore()

    def greet(semaphore, peer, peer_time):
        pl.semaphore_signal(
            semaphore, inc=1, device_id={"space": peer, "tm": peer_time}, device_id_type=MESH
        )

    for j in range(hubs):
        peer = j + n // 4
        pl.when((me != peer) | is_leaf)(functools.partial(greet, barrier, peer, hub_time))
    for other in range(times):
        for peer in list(range(n // 4)) + list(reversed(range(n // 4, n))):
            if n // 4 <= peer < n // 4 + hubs and other == times - 1:
                continue
            across = (line == peer // 2) & (side != peer % 2)
            above = (side == peer % 2) & (line < peer // 2)
            pl.when(is_hub | ((time == other) & (across | above)))(
                functools.partial(greet, barrier, peer, other)
            )
    lower = jnp.where(time == hub_time, (line == lines - 1).astype(jnp.int32), line)
    expected = jnp.where(is_hub, times * n - 1, hubs + 1 + lower)

    def remote(src, dst, recv, peer, peer_time=None):
        peer_time = time if peer_time is None else peer_time
        return pltpu.make_async_remote_copy(
            src_ref=src, dst_ref=dst, send_sem=send_sem.at[0], recv_sem=recv,
            device_id={"space": peer, "tm": peer_time}, device_id_type=MESH,
        )

    def arrived(ref, sem):
        pltpu.make_async_copy(ref, ref, sem).wait()

    def sink_of(owner):
        return sink.at[owner]

    late = line >= lines // 2
    toward = jnp.where(late, 1, -1)

    def enter():
        pl.semaphore_wait(barrier, expected)

        @pl.when(is_hub)
        def _():
            for other in range(times):
                greet(ready.at[0], me + 2 * toward, other)
                if other < times - 1:
                    greet(ready.at[0], me, other)

        for lower in range(lines - 1):
            pl.when((lower < line) & ((lower != 1) | (line < lines - 1)))(
                functools.partial(greet, reply.at[jnp.maximum(line, 1) - 1], 2 * lower + side, time)
            )

    def send_up(target):
        pl.semaphore_wait(reply.at[target - 1], 1)
        send_sink(target)

    def send_sink(target):
        remote(sink_of(me), sink_of(me), line_recv.at[line], 2 * target + side).start()

    def send_near():
        remote(sink_of(me), sink_of(me), near_recv.at[0], partner).start()

    load_momenta.wait()
    cosine, sine = site_phases(lambda i: momenta[0, i], me * sites, sites, extent_x, (sites, eig_count))
    waves[0] = cosine
    waves[1] = sine
    load_slots.wait()
    load_per.wait()
    sink[me] = per[slots[1]].reshape(8, rows, eig_count)

    early = late & (time == 0)

    @pl.when(early)
    def _():
        enter()
        send_sink(jnp.where(line == lines - 1, 0, 1))
        send_near()

    load_eig.wait()
    eig32[...] = eig[...].astype(F32)
    for color in range(3):
        real = eig32[pl.ds(2 * color, sites, stride=6), :]
        imag = eig32[pl.ds(2 * color + 1, sites, stride=6), :]
        wave_real = (waves[0] * real - waves[1] * imag).astype(BF16)
        wave_imag = (waves[1] * real + waves[0] * imag).astype(BF16)
        span = pl.ds(color * sites, sites)
        left[span, :eig_count] = real.astype(BF16)
        left[span, eig_count:] = imag.astype(BF16)
        right[span, :eig_count] = wave_real
        right[span, eig_count:] = wave_imag
    whole = lax.dot_general(
        left[...], right[...], (((0,), (0,)), ((), ())), preferred_element_type=F32
    )
    whole = jnp.concatenate(
        [
            whole[:eig_count, :eig_count] + whole[eig_count:, eig_count:],
            whole[:eig_count, eig_count:] - whole[eig_count:, :eig_count],
        ],
        axis=1,
    )
    part[...] = whole.astype(part.dtype).reshape(hubs, hub_rows, 2 * eig_count)

    def send_red():
        for i in range(hubs):
            j = 2 * (i // 2) + (1 - i % 2) * (1 - 2 * side) + side
            j = jnp.where(me < n // 2, (j + 2) % 4, j)
            copy = remote(
                part.at[j], sums.at[time * n + me], red_recv.at[time], j + n // 4, hub_time
            )
            pl.when((slot != j) | is_leaf)(copy.start)

    def send_turned():
        for k in range(1, n):
            peer = lax.rem(me + k, n)
            remote(turned.at[peer], picked.at[me], turn_recv.at[0], peer).start()

    pl.when(jnp.logical_not(early))(enter)
    send_red()

    @pl.when(jnp.logical_not(early))
    def _():
        send_near()
        pl.when((line == 1) | (line == lines - 1))(lambda: send_sink(0))
        pl.when(line == lines - 2)(lambda: send_sink(0))
        pl.when(line == lines - 2)(lambda: send_sink(1))

    load_columns.start()
    load_phases.start()
    first = per[slots[0]].reshape(8 * rows, eig_count).astype(F32)
    turned[...] = first.T.astype(BF16).reshape(n, rows, 8 * rows)
    picked[me] = turned[me]

    @pl.when(line < lines // 2)
    def _():
        pl.when(line == 0)(lambda: send_up(1))
        send_up(2)

    pl.when(is_leaf)(lambda: pl.semaphore_wait(ready.at[0], 1))
    send_turned()
    pl.when((line == 0) | (line == lines - 2))(lambda: send_up(lines - 1))
    pl.when(line == lines - 1)(lambda: send_sink(1))
    pl.when(line == lines - 1)(lambda: send_sink(2))

    def forward(origin):
        owner = 2 * origin + side
        arrived(sink.at[owner], line_recv.at[origin])
        return owner

    def pass_on(origin):
        owner = forward(origin)
        remote(sink.at[owner], sink.at[owner], near_recv.at[0], partner).start()

    inner_line = (line > 0) & (line < lines - 1)

    @pl.when(is_hub)
    def _():
        sums[time * n + me] = part[here]
        for other in range(times):
            own = other == times - 1
            if own:
                pl.when(line == 1)(lambda: pass_on(0))
            arrived(sums.at[pl.ds(0, n - own)], red_recv.at[other])
            total = sums[other * n].astype(F32)
            for k in range(1, n):
                total = total + sums[other * n + k].astype(F32)
            source = mfull.at[here] if own else spread.at[other]
            source[...] = total.astype(BF16)
            for k in range(n - own):
                peer = k + (k >= me).astype(jnp.int32) if own else k
                remote(source, mfull.at[here], all_recv.at[0], peer, other).start()

    relays = inner_line & (late | (time == 0))

    @pl.when(inner_line & jnp.logical_not(relays))
    def _():
        pass_on(line - toward)

    @pl.when(relays)
    def _():
        origin = line - toward
        owner = forward(origin)
        ends = me + 2 * toward
        block = sink.at[owner]
        remote(block, block, line_recv.at[line + toward], ends + 1 - 2 * side).start()
        remote(block, block, line_recv.at[origin], ends).start()
        remote(block, block, near_recv.at[0], partner).start()

    @pl.when(inner_line)
    def _():
        pl.when(late | (time < hub_time))(lambda: pass_on(line + toward))
        pass_on(line - 2 * toward)

    plain_end = (line == 0) & (time == hub_time)

    @pl.when(jnp.logical_not(inner_line))
    def _():
        pass_on(line - toward)
        pl.when(plain_end)(lambda: pass_on(line - 2 * toward))
        pass_on(line - 3 * toward)

    arrived(picked.at[pl.ds(0, n - 1)], turn_recv.at[0])
    group = lax.broadcasted_iota(jnp.int32, (rows, eig_count), 1) // rows
    chunks = [None] * 8
    for k in range(n):
        block = picked[k].astype(F32)
        for c in range(8):
            turn = (k - c) % 8
            moved = pltpu.roll(block, turn * rows, 1) if turn else block
            chunks[c] = moved if chunks[c] is None else jnp.where(group == k, moved, chunks[c])
    sources = jnp.concatenate(chunks[0::2] + chunks[1::2], axis=0).astype(BF16)
    load_columns.wait()
    load_phases.wait()
    for g in range(gammas):
        for spin in range(4):
            phase = phases[spin, g]
            place = spin * 4 + columns[spin, g]
            picks[0, 4 * g + spin] = phase * 16 + place
            picks[1, 4 * g + spin] = lax.rem(phase + 3, 4) * 16 + place

    @pl.when(inner_line | plain_end)
    def _():
        arrived(sink.at[pl.ds(0, lines)], near_recv.at[0])

    @pl.when(jnp.logical_not(inner_line | plain_end))
    def _():
        forward(line - 2 * toward)
        arrived(sink.at[me], line_recv.at[line])
        arrived(sink.at[pl.ds(0, lines - 1)], near_recv.at[0])

    @pl.when(is_hub)
    def _():
        arrived(mfull.at[pl.ds(0, hubs - 1)], all_recv.at[0])

    @pl.when(is_leaf)
    def _():
        arrived(mfull, all_recv.at[0])

    half = 4 * rows
    both = jnp.dot(sources, mfull[...].reshape(eig_count, 2 * eig_count), preferred_element_type=F32)
    cross_real = ((both[:half, :eig_count] + both[half:, eig_count:]) * factor).astype(BF16)
    cross_imag = ((both[:half, eig_count:] - both[half:, :eig_count]) * factor).astype(BF16)
    stacked = jnp.concatenate(
        [
            jnp.concatenate([cross_real, -cross_imag], axis=1),
            jnp.concatenate([cross_imag, cross_real], axis=1),
        ],
        axis=0,
    )
    for pair in range(2):
        table = jnp.concatenate(
            [
                jnp.concatenate(
                    [sink[owner, 4 * pair + 2 * i + c] for c in range(2) for owner in range(n)], axis=0
                )
                for i in range(2)
            ],
            axis=1,
        )
        result = jnp.dot(stacked, table, preferred_element_type=F32)
        for i in range(2):
            for spin in range(4):
                place = spin * 4 + 2 * pair + i
                columns_of = slice(i * eig_count, (i + 1) * eig_count)
                real = result[spin * rows : (spin + 1) * rows, columns_of]
                imag = result[(4 + spin) * rows : (5 + spin) * rows, columns_of]
                for turn, block in enumerate((real, -imag, -real, imag)):
                    blocks[turn * 16 + place] = block
    for g in range(gammas):
        for which in range(2):
            term = blocks[picks[which, 4 * g]]
            for spin in range(1, 4):
                term = term + blocks[picks[which, 4 * g + spin]]
            out_ref[pl.ds(2 * g + which, rows, stride=2 * gammas), :] = term

    unit = 4 * rows
    plain = hubs * unit + 2 * lines * 8 * rows + (n - 1) * rows - 8 * rows
    extra = (times * n - 2) * unit

    block = 8 * rows
    direct = time == hub_time
    changes = (
        (inner_line & (late | jnp.logical_not(direct)) & jnp.logical_not(late & direct), block),
        (late & inner_line & direct, 2 * block),
        (jnp.logical_not(late) & inner_line & direct, -block),
        (plain_end, 0),
        (jnp.logical_not(inner_line | plain_end), -block),
    )
    for hub, spreading in ((is_hub, extra), (is_leaf, 0)):
        for some, change in changes:
            pl.when(hub & some)(
                functools.partial(
                    arrived, volume.at[pl.ds(0, plain + spreading + change)], send_sem.at[0]
                )
            )


def store_kernel(source, target, sem):
    copy = pltpu.make_async_copy(source, target, sem.at[0])
    copy.start()
    copy.wait()


def on_device_kernel(eigvecs, perambulator, momenta, source_slots, gamma_columns, gamma_phases):
    sites, eig_count = eigvecs.shape[1], eigvecs.shape[4]
    n = lax.axis_size("space")
    times = lax.axis_size("tm")
    rows = eig_count // n
    total_sites = sites * n
    gammas = gamma_columns.shape[0]
    stored = perambulator.shape[1]
    body = functools.partial(
        kernel, n, sites, total_sites // (LY * LZ), 1.0 / math.sqrt(12.0 * total_sites)
    )
    dma = pltpu.SemaphoreType.DMA
    hbm = pl.BlockSpec(memory_space=pltpu.HBM)
    out = pl.pallas_call(
        body,
        out_shape=pltpu.VMEM((rows * gammas * 2, eig_count), F32),
        in_specs=[hbm] * 6,
        out_specs=pl.BlockSpec(memory_space=pltpu.VMEM),
        scratch_shapes=[
            pltpu.SMEM(momenta.shape, jnp.int32),
            pltpu.SMEM(source_slots.shape, jnp.int32),
            pltpu.SMEM((4, gammas), jnp.int32),
            pltpu.SMEM((4, gammas), jnp.int32),
            pltpu.SMEM((2, 4 * gammas), jnp.int32),
            pltpu.VMEM((sites * 6, eig_count), BF16),
            pltpu.VMEM((sites * 6, eig_count), F32),
            pltpu.VMEM((2, sites, eig_count), F32),
            pltpu.VMEM((sites * 3, 2 * eig_count), BF16),
            pltpu.VMEM((sites * 3, 2 * eig_count), BF16),
            pltpu.VMEM((stored, 4, 2, rows, eig_count), BF16),
            pltpu.VMEM((n, 8, rows, eig_count), BF16),
            pltpu.VMEM((n, rows, 8 * rows), BF16),
            pltpu.VMEM((n, rows, 8 * rows), BF16),
            pltpu.VMEM((n // 2, 2 * rows, 2 * eig_count), WIRE),
            pltpu.VMEM((times * n, 2 * rows, 2 * eig_count), WIRE),
            pltpu.VMEM((times - 1, 2 * rows, 2 * eig_count), BF16),
            pltpu.VMEM((n // 2, 2 * rows, 2 * eig_count), BF16),
            pltpu.VMEM((64, rows, eig_count), F32),
            pltpu.VMEM((24 * eig_count, eig_count), BF16),
            pltpu.SemaphoreType.REGULAR((1,)),
            pltpu.SemaphoreType.REGULAR((n // 2 - 1,)),
            dma((4,)),
            dma((1,)),
            dma((2,)),
            dma((1,)),
            dma((1,)),
            dma((1,)),
            dma((n // 2,)),
        ],
        compiler_params=pltpu.CompilerParams(
            collective_id=0, has_side_effects=True, vmem_limit_bytes=VMEM_LIMIT
        ),
    )(
        *(
            pltpu.with_memory_space_constraint(array, pltpu.HBM)
            for array in (
                momenta,
                source_slots,
                gamma_columns.T,
                gamma_phases.T,
                eigvecs.reshape(sites * 6, eig_count),
                perambulator[0],
            )
        )
    )
    done = pl.pallas_call(
        store_kernel,
        out_shape=jax.ShapeDtypeStruct(out.shape, F32),
        in_specs=[pl.BlockSpec(memory_space=pl.ANY)],
        out_specs=hbm,
        scratch_shapes=[dma((1,))],
        compiler_params=pltpu.CompilerParams(vmem_limit_bytes=VMEM_LIMIT),
    )(out)
    return done.reshape(1, rows, 1, gammas, 2, eig_count)


def on_device_plain(eigvecs, perambulator, momenta, source_slots, gamma_columns, gamma_phases):
    sites, eig_count = eigvecs.shape[1], eigvecs.shape[4]
    n = lax.axis_size("space")
    total_sites = sites * n
    extent_x = total_sites // (LY * LZ)
    factor = 1.0 / math.sqrt(12.0 * total_sites)
    first_site = lax.axis_index("space") * sites
    chosen = jnp.take(perambulator[0], source_slots, axis=0)
    sinks = lax.all_gather(chosen[1], "space", axis=2, tiled=True)
    turned = lax.all_to_all(chosen[0], "space", split_axis=3, concat_axis=2, tiled=True)
    real = eigvecs[0, :, :, 0].astype(F32)
    imag = eigvecs[0, :, :, 1].astype(F32)
    flat = eigvecs[0].reshape(sites * 6, eig_count)
    tables = []
    for p in range(momenta.shape[0]):
        cosine, sine = site_phases(
            lambda i, p=p: momenta[p, i], first_site, sites, extent_x, (sites, 1, 1)
        )
        wave_real = cosine * real - sine * imag
        wave_imag = sine * real + cosine * imag
        upper = jnp.concatenate([wave_real, wave_imag], axis=2)
        lower = jnp.concatenate([wave_imag, -wave_real], axis=2)
        waves = jnp.stack([upper, lower], axis=2).astype(BF16).reshape(sites * 6, 2 * eig_count)
        tables.append(
            lax.dot_general(flat, waves, (((0,), (0,)), ((), ())), preferred_element_type=F32)
        )
    whole = lax.psum(jnp.stack(tables), "space").astype(BF16)
    turned_whole = jnp.concatenate([whole[:, :, eig_count:], -whole[:, :, :eig_count]], axis=2)
    both = jnp.stack([whole, turned_whole], axis=1)
    cross = jnp.einsum("skla,pklm->aspm", turned, both, preferred_element_type=F32)
    cross_real, cross_imag = cross[..., :eig_count], cross[..., eig_count:]
    stacked = jnp.stack(
        [
            jnp.stack([cross_real, -cross_imag], axis=-2),
            jnp.stack([cross_imag, cross_real], axis=-2),
        ],
        axis=3,
    ).astype(BF16)
    blocks = jnp.einsum("asphkl,tklb->apsthb", stacked, sinks, preferred_element_type=F32)
    spins = jnp.arange(4, dtype=jnp.int32)
    matches = (gamma_columns[:, :, None] == spins).astype(F32)
    real_sign = (gamma_phases == 0).astype(F32) - (gamma_phases == 2).astype(F32)
    imag_sign = (gamma_phases == 1).astype(F32) - (gamma_phases == 3).astype(F32)
    mix_real = matches * real_sign[:, :, None]
    mix_imag = matches * imag_sign[:, :, None]
    mix = jnp.stack(
        [jnp.stack([mix_real, -mix_imag], axis=-1), jnp.stack([mix_imag, mix_real], axis=-1)],
        axis=1,
    )
    meson = factor * jnp.einsum("gosth,apsthb->apgob", mix, blocks, precision=lax.Precision.HIGHEST)
    return meson[None]


def on_device(eigvecs, perambulator, momenta, *rest):
    n = lax.axis_size("space")
    rows = perambulator.shape[4]
    small = eigvecs.shape[1] % 16 == 0 and eigvecs.shape[4] == 128
    if rows == 16 and n == 8 and lax.axis_size("tm") == 2 and momenta.shape[0] == 1 and small:
        return on_device_kernel(eigvecs, perambulator, momenta, *rest)
    return on_device_plain(eigvecs, perambulator, momenta, *rest)


def solution(mesh):
    in_specs = (
        P(("cfg", "tm"), "space", None, None, None),
        P(("cfg", "tm"), None, None, None, "space", None),
        P(),
        P(),
        P(),
        P(),
    )
    out_specs = P(("cfg", "tm"), "space", None, None, None, None)
    return jax.shard_map(
        on_device, mesh=mesh, in_specs=in_specs, out_specs=out_specs, check_vma=False
    )
```

```python
import functools
import math

import jax
import jax.numpy as jnp
from jax import lax
from jax.experimental import pallas as pl
from jax.experimental.pallas import tpu as pltpu
from jax.sharding import PartitionSpec as P

LY = 48
LZ = 48
WIRE = jnp.bfloat16
F32 = jnp.float32
BF16 = jnp.bfloat16
MESH = pl.DeviceIdType.MESH
VMEM_LIMIT = 32 * 1024 * 1024


def site_coords(first_site, shape):
    site = (lax.broadcasted_iota(jnp.int32, shape, 0) + first_site).astype(F32)
    lines = jnp.floor((site + 0.5) * (1.0 / LZ))
    coord_x = jnp.floor((lines + 0.5) * (1.0 / LY))
    coord_y = lines - LY * coord_x
    coord_z = site - LZ * lines
    return coord_x, coord_y, coord_z


def site_phases(momenta_at, coords, extent_x, shape):
    coord_x, coord_y, coord_z = coords

    def share(momentum, coord, extent):
        turn = momentum.astype(F32) * coord * (1.0 / extent)
        return turn - jnp.floor(turn)

    turns = (
        share(momenta_at(0), coord_x, extent_x)
        + share(momenta_at(1), coord_y, LY)
        + share(momenta_at(2), coord_z, LZ)
    )
    turns = turns - jnp.floor(turns + 0.5)
    half = math.pi * turns
    square = half * half
    sine = jnp.full(shape, 1.0 / 6227020800.0, F32)
    for term in (-1.0 / 39916800.0, 1.0 / 362880.0, -1.0 / 5040.0, 1.0 / 120.0, -1.0 / 6.0, 1.0):
        sine = sine * square + term
    sine = sine * half
    cosine = jnp.full(shape, 1.0 / 479001600.0, F32)
    for term in (-1.0 / 3628800.0, 1.0 / 40320.0, -1.0 / 720.0, 1.0 / 24.0, -0.5, 1.0):
        cosine = cosine * square + term
    return 1.0 - 2.0 * sine * sine, 2.0 * sine * cosine


def kernel(
    n, sites, extent_x, factor,
    momenta_hbm, slots_hbm, columns_hbm, phases_hbm, eig_hbm, per_hbm, out_ref,
    momenta, slots, columns, phases, picks, eig, eig32, coords, waves, left, right, per, sink, turned, picked,
    part, sums, spread, mfull, blocks, volume,
    ready, reply, load_sem, send_sem, red_recv, all_recv, turn_recv, near_recv, line_recv,
):
    me = lax.axis_index("space")
    time = lax.axis_index("tm")
    times = lax.axis_size("tm")
    hub_time = times - 1
    eig_count = eig.shape[1]
    rows = eig_count // n
    gammas = columns.shape[1]
    hubs = n // 2
    hub_rows = eig_count // hubs
    slot = me - n // 4
    inner = (slot >= 0) & (slot < hubs)
    is_hub = inner & (time == hub_time)
    is_leaf = jnp.logical_not(is_hub)
    here = jnp.clip(slot, 0, hubs - 1)
    side = lax.rem(me, 2)
    line = lax.div(me, 2)
    lines = n // 2
    partner = me + 1 - 2 * side

    load_per = pltpu.make_async_copy(per_hbm, per, load_sem.at[0])
    load_eig = pltpu.make_async_copy(eig_hbm, eig, load_sem.at[1])
    load_slots = pltpu.make_async_copy(slots_hbm, slots, load_sem.at[2])
    load_momenta = pltpu.make_async_copy(momenta_hbm, momenta, load_sem.at[3])
    load_columns = pltpu.make_async_copy(columns_hbm, columns, load_sem.at[2])
    load_phases = pltpu.make_async_copy(phases_hbm, phases, load_sem.at[3])
    for load in (load_slots, load_momenta, load_per, load_eig):
        load.start()

    barrier = pltpu.get_barrier_semaphore()

    def greet(semaphore, peer, peer_time):
        pl.semaphore_signal(
            semaphore, inc=1, device_id={"space": peer, "tm": peer_time}, device_id_type=MESH
        )

    for j in range(hubs):
        peer = j + n // 4
        pl.when((me != peer) | is_leaf)(functools.partial(greet, barrier, peer, hub_time))
    for other in range(times):
        for peer in list(range(n // 4)) + list(reversed(range(n // 4, n))):
            if n // 4 <= peer < n // 4 + hubs and other == times - 1:
                continue
            across = (line == peer // 2) & (side != peer % 2)
            above = (side == peer % 2) & (line < peer // 2)
            pl.when(is_hub | ((time == other) & (across | above)))(
                functools.partial(greet, barrier, peer, other)
            )
    lower = jnp.where(time == hub_time, (line == lines - 1).astype(jnp.int32), line)
    expected = jnp.where(is_hub, times * n - 1, hubs + 1 + lower)

    def remote(src, dst, recv, peer, peer_time=None):
        peer_time = time if peer_time is None else peer_time
        return pltpu.make_async_remote_copy(
            src_ref=src, dst_ref=dst, send_sem=send_sem.at[0], recv_sem=recv,
            device_id={"space": peer, "tm": peer_time}, device_id_type=MESH,
        )

    def arrived(ref, sem):
        pltpu.make_async_copy(ref, ref, sem).wait()

    def sink_of(owner):
        return sink.at[owner]

    late = line >= lines // 2
    toward = jnp.where(late, 1, -1)

    def enter():
        pl.semaphore_wait(barrier, expected)

        @pl.when(is_hub)
        def _():
            for other in range(times):
                greet(ready.at[0], me + 2 * toward, other)
                if other < times - 1:
                    greet(ready.at[0], me, other)

        for lower in range(lines - 1):
            pl.when((lower < line) & ((lower != 1) | (line < lines - 1)))(
                functools.partial(greet, reply.at[jnp.maximum(line, 1) - 1], 2 * lower + side, time)
            )

    def send_up(target):
        pl.semaphore_wait(reply.at[target - 1], 1)
        send_sink(target)

    def send_sink(target):
        remote(sink_of(me), sink_of(me), line_recv.at[line], 2 * target + side).start()

    def send_near():
        remote(sink_of(me), sink_of(me), near_recv.at[0], partner).start()

    for i, coord in enumerate(site_coords(me * sites, (sites, eig_count))):
        coords[i] = coord
    load_momenta.wait()
    cosine, sine = site_phases(
        lambda i: momenta[0, i], [coords[i] for i in range(3)], extent_x, (sites, eig_count)
    )
    waves[0] = cosine
    waves[1] = sine
    load_slots.wait()
    load_per.wait()
    sink[me] = per[slots[1]].reshape(8, rows, eig_count)

    early = late & (time == 0)

    @pl.when(early)
    def _():
        enter()
        send_sink(jnp.where(line == lines - 1, 0, 1))
        send_near()

    load_eig.wait()
    eig32[...] = eig[...].astype(F32)
    for color in range(3):
        real = eig32[pl.ds(2 * color, sites, stride=6), :]
        imag = eig32[pl.ds(2 * color + 1, sites, stride=6), :]
        wave_real = (waves[0] * real - waves[1] * imag).astype(BF16)
        wave_imag = (waves[1] * real + waves[0] * imag).astype(BF16)
        span = pl.ds(color * sites, sites)
        left[span, :eig_count] = real.astype(BF16)
        left[span, eig_count:] = imag.astype(BF16)
        right[span, :eig_count] = wave_real
        right[span, eig_count:] = wave_imag
    whole = lax.dot_general(
        left[...], right[...], (((0,), (0,)), ((), ())), preferred_element_type=F32
    )
    whole = jnp.concatenate(
        [
            whole[:eig_count, :eig_count] + whole[eig_count:, eig_count:],
            whole[:eig_count, eig_count:] - whole[eig_count:, :eig_count],
        ],
        axis=1,
    )
    part[...] = whole.astype(part.dtype).reshape(hubs, hub_rows, 2 * eig_count)

    def send_red():
        for i in range(hubs):
            j = 2 * (i // 2) + (1 - i % 2) * (1 - 2 * side) + side
            j = jnp.where(me < n // 2, (j + 2) % 4, j)
            copy = remote(
                part.at[j], sums.at[time * n + me], red_recv.at[time], j + n // 4, hub_time
            )
            pl.when((slot != j) | is_leaf)(copy.start)

    def send_turned():
        for k in range(1, n):
            peer = lax.rem(me + k, n)
            remote(turned.at[peer], picked.at[me], turn_recv.at[0], peer).start()

    pl.when(jnp.logical_not(early))(enter)
    send_red()

    @pl.when(jnp.logical_not(early))
    def _():
        send_near()
        pl.when((line == 1) | (line == lines - 1))(lambda: send_sink(0))
        pl.when(line == lines - 2)(lambda: send_sink(0))
        pl.when(line == lines - 2)(lambda: send_sink(1))

    load_columns.start()
    load_phases.start()
    first = per[slots[0]].reshape(8 * rows, eig_count).astype(F32)
    turned[...] = first.T.astype(BF16).reshape(n, rows, 8 * rows)
    picked[me] = turned[me]

    @pl.when(line < lines // 2)
    def _():
        pl.when(line == 0)(lambda: send_up(1))
        send_up(2)

    pl.when(is_leaf)(lambda: pl.semaphore_wait(ready.at[0], 1))
    send_turned()
    pl.when((line == 0) | (line == lines - 2))(lambda: send_up(lines - 1))
    pl.when(line == lines - 1)(lambda: send_sink(1))
    pl.when(line == lines - 1)(lambda: send_sink(2))

    def forward(origin):
        owner = 2 * origin + side
        arrived(sink.at[owner], line_recv.at[origin])
        return owner

    def pass_on(origin):
        owner = forward(origin)
        remote(sink.at[owner], sink.at[owner], near_recv.at[0], partner).start()

    inner_line = (line > 0) & (line < lines - 1)

    @pl.when(is_hub)
    def _():
        sums[time * n + me] = part[here]
        for other in range(times):
            own = other == times - 1
            if own:
                pl.when(line == 1)(lambda: pass_on(0))
            arrived(sums.at[pl.ds(0, n - own)], red_recv.at[other])
            total = sums[other * n].astype(F32)
            for k in range(1, n):
                total = total + sums[other * n + k].astype(F32)
            source = mfull.at[here] if own else spread.at[other]
            source[...] = total.astype(BF16)
            for k in range(n - own):
                peer = k + (k >= me).astype(jnp.int32) if own else k
                remote(source, mfull.at[here], all_recv.at[0], peer, other).start()

    relays = inner_line & (late | (time == 0))

    @pl.when(inner_line & jnp.logical_not(relays))
    def _():
        pass_on(line - toward)

    @pl.when(relays)
    def _():
        origin = line - toward
        owner = forward(origin)
        ends = me + 2 * toward
        block = sink.at[owner]
        remote(block, block, line_recv.at[line + toward], ends + 1 - 2 * side).start()
        remote(block, block, line_recv.at[origin], ends).start()
        remote(block, block, near_recv.at[0], partner).start()

    @pl.when(inner_line)
    def _():
        pl.when(late | (time < hub_time))(lambda: pass_on(line + toward))
        pass_on(line - 2 * toward)

    plain_end = (line == 0) & (time == hub_time)

    @pl.when(jnp.logical_not(inner_line))
    def _():
        pass_on(line - toward)
        pl.when(plain_end)(lambda: pass_on(line - 2 * toward))
        pass_on(line - 3 * toward)

    arrived(picked.at[pl.ds(0, n - 1)], turn_recv.at[0])
    group = lax.broadcasted_iota(jnp.int32, (rows, eig_count), 1) // rows
    chunks = [None] * 8
    for k in range(n):
        block = picked[k].astype(F32)
        for c in range(8):
            turn = (k - c) % 8
            moved = pltpu.roll(block, turn * rows, 1) if turn else block
            chunks[c] = moved if chunks[c] is None else jnp.where(group == k, moved, chunks[c])
    sources = jnp.concatenate(chunks[0::2] + chunks[1::2], axis=0).astype(BF16)
    load_columns.wait()
    load_phases.wait()
    for g in range(gammas):
        for spin in range(4):
            phase = phases[spin, g]
            place = spin * 4 + columns[spin, g]
            picks[0, 4 * g + spin] = phase * 16 + place
            picks[1, 4 * g + spin] = lax.rem(phase + 3, 4) * 16 + place

    @pl.when(inner_line | plain_end)
    def _():
        arrived(sink.at[pl.ds(0, lines)], near_recv.at[0])

    @pl.when(jnp.logical_not(inner_line | plain_end))
    def _():
        forward(line - 2 * toward)
        arrived(sink.at[me], line_recv.at[line])
        arrived(sink.at[pl.ds(0, lines - 1)], near_recv.at[0])

    @pl.when(is_hub)
    def _():
        arrived(mfull.at[pl.ds(0, hubs - 1)], all_recv.at[0])

    @pl.when(is_leaf)
    def _():
        arrived(mfull, all_recv.at[0])

    half = 4 * rows
    both = jnp.dot(sources, mfull[...].reshape(eig_count, 2 * eig_count), preferred_element_type=F32)
    cross_real = ((both[:half, :eig_count] + both[half:, eig_count:]) * factor).astype(BF16)
    cross_imag = ((both[:half, eig_count:] - both[half:, :eig_count]) * factor).astype(BF16)
    stacked = jnp.concatenate(
        [
            jnp.concatenate([cross_real, -cross_imag], axis=1),
            jnp.concatenate([cross_imag, cross_real], axis=1),
        ],
        axis=0,
    )
    for pair in range(2):
        table = jnp.concatenate(
            [
                jnp.concatenate(
                    [sink[owner, 4 * pair + 2 * i + c] for c in range(2) for owner in range(n)], axis=0
                )
                for i in range(2)
            ],
            axis=1,
        )
        result = jnp.dot(stacked, table, preferred_element_type=F32)
        for i in range(2):
            for spin in range(4):
                place = spin * 4 + 2 * pair + i
                columns_of = slice(i * eig_count, (i + 1) * eig_count)
                real = result[spin * rows : (spin + 1) * rows, columns_of]
                imag = result[(4 + spin) * rows : (5 + spin) * rows, columns_of]
                for turn, block in enumerate((real, -imag, -real, imag)):
                    blocks[turn * 16 + place] = block
    for g in range(gammas):
        for which in range(2):
            term = blocks[picks[which, 4 * g]]
            for spin in range(1, 4):
                term = term + blocks[picks[which, 4 * g + spin]]
            out_ref[pl.ds(2 * g + which, rows, stride=2 * gammas), :] = term

    unit = 4 * rows
    plain = hubs * unit + 2 * lines * 8 * rows + (n - 1) * rows - 8 * rows
    extra = (times * n - 2) * unit

    block = 8 * rows
    direct = time == hub_time
    changes = (
        (inner_line & (late | jnp.logical_not(direct)) & jnp.logical_not(late & direct), block),
        (late & inner_line & direct, 2 * block),
        (jnp.logical_not(late) & inner_line & direct, -block),
        (plain_end, 0),
        (jnp.logical_not(inner_line | plain_end), -block),
    )
    for hub, spreading in ((is_hub, extra), (is_leaf, 0)):
        for some, change in changes:
            pl.when(hub & some)(
                functools.partial(
                    arrived, volume.at[pl.ds(0, plain + spreading + change)], send_sem.at[0]
                )
            )


def store_kernel(source, target, sem):
    copy = pltpu.make_async_copy(source, target, sem.at[0])
    copy.start()
    copy.wait()


def on_device_kernel(eigvecs, perambulator, momenta, source_slots, gamma_columns, gamma_phases):
    sites, eig_count = eigvecs.shape[1], eigvecs.shape[4]
    n = lax.axis_size("space")
    times = lax.axis_size("tm")
    rows = eig_count // n
    total_sites = sites * n
    gammas = gamma_columns.shape[0]
    stored = perambulator.shape[1]
    body = functools.partial(
        kernel, n, sites, total_sites // (LY * LZ), 1.0 / math.sqrt(12.0 * total_sites)
    )
    dma = pltpu.SemaphoreType.DMA
    hbm = pl.BlockSpec(memory_space=pltpu.HBM)
    out = pl.pallas_call(
        body,
        out_shape=pltpu.VMEM((rows * gammas * 2, eig_count), F32),
        in_specs=[hbm] * 6,
        out_specs=pl.BlockSpec(memory_space=pltpu.VMEM),
        scratch_shapes=[
            pltpu.SMEM(momenta.shape, jnp.int32),
            pltpu.SMEM(source_slots.shape, jnp.int32),
            pltpu.SMEM((4, gammas), jnp.int32),
            pltpu.SMEM((4, gammas), jnp.int32),
            pltpu.SMEM((2, 4 * gammas), jnp.int32),
            pltpu.VMEM((sites * 6, eig_count), BF16),
            pltpu.VMEM((sites * 6, eig_count), F32),
            pltpu.VMEM((3, sites, eig_count), F32),
            pltpu.VMEM((2, sites, eig_count), F32),
            pltpu.VMEM((sites * 3, 2 * eig_count), BF16),
            pltpu.VMEM((sites * 3, 2 * eig_count), BF16),
            pltpu.VMEM((stored, 4, 2, rows, eig_count), BF16),
            pltpu.VMEM((n, 8, rows, eig_count), BF16),
            pltpu.VMEM((n, rows, 8 * rows), BF16),
            pltpu.VMEM((n, rows, 8 * rows), BF16),
            pltpu.VMEM((n // 2, 2 * rows, 2 * eig_count), WIRE),
            pltpu.VMEM((times * n, 2 * rows, 2 * eig_count), WIRE),
            pltpu.VMEM((times - 1, 2 * rows, 2 * eig_count), BF16),
            pltpu.VMEM((n // 2, 2 * rows, 2 * eig_count), BF16),
            pltpu.VMEM((64, rows, eig_count), F32),
            pltpu.VMEM((24 * eig_count, eig_count), BF16),
            pltpu.SemaphoreType.REGULAR((1,)),
            pltpu.SemaphoreType.REGULAR((n // 2 - 1,)),
            dma((4,)),
            dma((1,)),
            dma((2,)),
            dma((1,)),
            dma((1,)),
            dma((1,)),
            dma((n // 2,)),
        ],
        compiler_params=pltpu.CompilerParams(
            collective_id=0, has_side_effects=True, vmem_limit_bytes=VMEM_LIMIT
        ),
    )(
        *(
            pltpu.with_memory_space_constraint(array, pltpu.HBM)
            for array in (
                momenta,
                source_slots,
                gamma_columns.T,
                gamma_phases.T,
                eigvecs.reshape(sites * 6, eig_count),
                perambulator[0],
            )
        )
    )
    done = pl.pallas_call(
        store_kernel,
        out_shape=jax.ShapeDtypeStruct(out.shape, F32),
        in_specs=[pl.BlockSpec(memory_space=pl.ANY)],
        out_specs=hbm,
        scratch_shapes=[dma((1,))],
        compiler_params=pltpu.CompilerParams(vmem_limit_bytes=VMEM_LIMIT),
    )(out)
    return done.reshape(1, rows, 1, gammas, 2, eig_count)


def on_device_plain(eigvecs, perambulator, momenta, source_slots, gamma_columns, gamma_phases):
    sites, eig_count = eigvecs.shape[1], eigvecs.shape[4]
    n = lax.axis_size("space")
    total_sites = sites * n
    extent_x = total_sites // (LY * LZ)
    factor = 1.0 / math.sqrt(12.0 * total_sites)
    first_site = lax.axis_index("space") * sites
    chosen = jnp.take(perambulator[0], source_slots, axis=0)
    sinks = lax.all_gather(chosen[1], "space", axis=2, tiled=True)
    turned = lax.all_to_all(chosen[0], "space", split_axis=3, concat_axis=2, tiled=True)
    real = eigvecs[0, :, :, 0].astype(F32)
    imag = eigvecs[0, :, :, 1].astype(F32)
    flat = eigvecs[0].reshape(sites * 6, eig_count)
    tables = []
    for p in range(momenta.shape[0]):
        cosine, sine = site_phases(
            lambda i, p=p: momenta[p, i], site_coords(first_site, (sites, 1, 1)), extent_x, (sites, 1, 1)
        )
        wave_real = cosine * real - sine * imag
        wave_imag = sine * real + cosine * imag
        upper = jnp.concatenate([wave_real, wave_imag], axis=2)
        lower = jnp.concatenate([wave_imag, -wave_real], axis=2)
        waves = jnp.stack([upper, lower], axis=2).astype(BF16).reshape(sites * 6, 2 * eig_count)
        tables.append(
            lax.dot_general(flat, waves, (((0,), (0,)), ((), ())), preferred_element_type=F32)
        )
    whole = lax.psum(jnp.stack(tables), "space").astype(BF16)
    turned_whole = jnp.concatenate([whole[:, :, eig_count:], -whole[:, :, :eig_count]], axis=2)
    both = jnp.stack([whole, turned_whole], axis=1)
    cross = jnp.einsum("skla,pklm->aspm", turned, both, preferred_element_type=F32)
    cross_real, cross_imag = cross[..., :eig_count], cross[..., eig_count:]
    stacked = jnp.stack(
        [
            jnp.stack([cross_real, -cross_imag], axis=-2),
            jnp.stack([cross_imag, cross_real], axis=-2),
        ],
        axis=3,
    ).astype(BF16)
    blocks = jnp.einsum("asphkl,tklb->apsthb", stacked, sinks, preferred_element_type=F32)
    spins = jnp.arange(4, dtype=jnp.int32)
    matches = (gamma_columns[:, :, None] == spins).astype(F32)
    real_sign = (gamma_phases == 0).astype(F32) - (gamma_phases == 2).astype(F32)
    imag_sign = (gamma_phases == 1).astype(F32) - (gamma_phases == 3).astype(F32)
    mix_real = matches * real_sign[:, :, None]
    mix_imag = matches * imag_sign[:, :, None]
    mix = jnp.stack(
        [jnp.stack([mix_real, -mix_imag], axis=-1), jnp.stack([mix_imag, mix_real], axis=-1)],
        axis=1,
    )
    meson = factor * jnp.einsum("gosth,apsthb->apgob", mix, blocks, precision=lax.Precision.HIGHEST)
    return meson[None]


def on_device(eigvecs, perambulator, momenta, *rest):
    n = lax.axis_size("space")
    rows = perambulator.shape[4]
    small = eigvecs.shape[1] % 16 == 0 and eigvecs.shape[4] == 128
    if rows == 16 and n == 8 and lax.axis_size("tm") == 2 and momenta.shape[0] == 1 and small:
        return on_device_kernel(eigvecs, perambulator, momenta, *rest)
    return on_device_plain(eigvecs, perambulator, momenta, *rest)


def solution(mesh):
    in_specs = (
        P(("cfg", "tm"), "space", None, None, None),
        P(("cfg", "tm"), None, None, None, "space", None),
        P(),
        P(),
        P(),
        P(),
    )
    out_specs = P(("cfg", "tm"), "space", None, None, None, None)
    return jax.shard_map(
        on_device, mesh=mesh, in_specs=in_specs, out_specs=out_specs, check_vma=False
    )
```

```python
import functools
import math

import jax
import jax.numpy as jnp
from jax import lax
from jax.experimental import pallas as pl
from jax.experimental.pallas import tpu as pltpu
from jax.sharding import PartitionSpec as P

LY = 48
LZ = 48
WIRE = jnp.bfloat16
F32 = jnp.float32
BF16 = jnp.bfloat16
MESH = pl.DeviceIdType.MESH
VMEM_LIMIT = 32 * 1024 * 1024


def site_coords(first_site, shape):
    site = (lax.broadcasted_iota(jnp.int32, shape, 0) + first_site).astype(F32)
    lines = jnp.floor((site + 0.5) * (1.0 / LZ))
    coord_x = jnp.floor((lines + 0.5) * (1.0 / LY))
    coord_y = lines - LY * coord_x
    coord_z = site - LZ * lines
    return coord_x, coord_y, coord_z


def site_phases(momenta_at, coords, extent_x, shape):
    coord_x, coord_y, coord_z = coords

    def share(momentum, coord, extent):
        turn = momentum.astype(F32) * coord * (1.0 / extent)
        return turn - jnp.floor(turn)

    turns = (
        share(momenta_at(0), coord_x, extent_x)
        + share(momenta_at(1), coord_y, LY)
        + share(momenta_at(2), coord_z, LZ)
    )
    turns = turns - jnp.floor(turns + 0.5)
    half = math.pi * turns
    square = half * half
    sine = jnp.full(shape, 1.0 / 6227020800.0, F32)
    for term in (-1.0 / 39916800.0, 1.0 / 362880.0, -1.0 / 5040.0, 1.0 / 120.0, -1.0 / 6.0, 1.0):
        sine = sine * square + term
    sine = sine * half
    cosine = jnp.full(shape, 1.0 / 479001600.0, F32)
    for term in (-1.0 / 3628800.0, 1.0 / 40320.0, -1.0 / 720.0, 1.0 / 24.0, -0.5, 1.0):
        cosine = cosine * square + term
    return 1.0 - 2.0 * sine * sine, 2.0 * sine * cosine


def kernel(
    n, sites, extent_x, factor,
    momenta_hbm, slots_hbm, columns_hbm, phases_hbm, eig_hbm, per_hbm, out_ref,
    momenta, slots, columns, phases, picks, eig, eig32, coords, waves, left, right, per, sink, turned, picked,
    part, sums, spread, mfull, blocks, volume,
    ready, reply, load_sem, send_sem, red_recv, all_recv, turn_recv, near_recv, line_recv,
):
    me = lax.axis_index("space")
    time = lax.axis_index("tm")
    times = lax.axis_size("tm")
    hub_time = times - 1
    eig_count = eig.shape[1]
    rows = eig_count // n
    gammas = columns.shape[1]
    hubs = n // 2
    hub_rows = eig_count // hubs
    slot = me - n // 4
    inner = (slot >= 0) & (slot < hubs)
    is_hub = inner & (time == hub_time)
    is_leaf = jnp.logical_not(is_hub)
    here = jnp.clip(slot, 0, hubs - 1)
    side = lax.rem(me, 2)
    line = lax.div(me, 2)
    lines = n // 2
    partner = me + 1 - 2 * side

    load_per = pltpu.make_async_copy(per_hbm, per, load_sem.at[0])
    load_eig = pltpu.make_async_copy(eig_hbm, eig, load_sem.at[1])
    load_slots = pltpu.make_async_copy(slots_hbm, slots, load_sem.at[2])
    load_momenta = pltpu.make_async_copy(momenta_hbm, momenta, load_sem.at[3])
    load_columns = pltpu.make_async_copy(columns_hbm, columns, load_sem.at[2])
    load_phases = pltpu.make_async_copy(phases_hbm, phases, load_sem.at[3])
    for load in (load_slots, load_momenta, load_per, load_eig):
        load.start()

    barrier = pltpu.get_barrier_semaphore()

    def greet(semaphore, peer, peer_time):
        pl.semaphore_signal(
            semaphore, inc=1, device_id={"space": peer, "tm": peer_time}, device_id_type=MESH
        )

    for j in range(hubs):
        peer = j + n // 4
        pl.when((me != peer) | is_leaf)(functools.partial(greet, barrier, peer, hub_time))
    for other in range(times):
        for peer in list(range(n // 4)) + list(reversed(range(n // 4, n))):
            if n // 4 <= peer < n // 4 + hubs and other == times - 1:
                continue
            across = (line == peer // 2) & (side != peer % 2)
            above = (side == peer % 2) & (line < peer // 2)
            pl.when(is_hub | ((time == other) & (across | above)))(
                functools.partial(greet, barrier, peer, other)
            )
    lower = jnp.where(time == hub_time, (line == lines - 1).astype(jnp.int32), line)
    expected = jnp.where(is_hub, times * n - 1, hubs + 1 + lower)

    def remote(src, dst, recv, peer, peer_time=None):
        peer_time = time if peer_time is None else peer_time
        return pltpu.make_async_remote_copy(
            src_ref=src, dst_ref=dst, send_sem=send_sem.at[0], recv_sem=recv,
            device_id={"space": peer, "tm": peer_time}, device_id_type=MESH,
        )

    def arrived(ref, sem):
        pltpu.make_async_copy(ref, ref, sem).wait()

    def sink_of(owner):
        return sink.at[owner]

    late = line >= lines // 2
    toward = jnp.where(late, 1, -1)

    def enter():
        pl.semaphore_wait(barrier, expected)

        @pl.when(is_hub)
        def _():
            for other in range(times):
                greet(ready.at[0], me + 2 * toward, other)
                if other < times - 1:
                    greet(ready.at[0], me, other)

        for lower in range(lines - 1):
            pl.when((lower < line) & ((lower != 1) | (line < lines - 1)))(
                functools.partial(greet, reply.at[jnp.maximum(line, 1) - 1], 2 * lower + side, time)
            )

    def send_up(target):
        pl.semaphore_wait(reply.at[target - 1], 1)
        send_sink(target)

    def send_sink(target):
        remote(sink_of(me), sink_of(me), line_recv.at[line], 2 * target + side).start()

    def send_near():
        remote(sink_of(me), sink_of(me), near_recv.at[0], partner).start()

    for i, coord in enumerate(site_coords(me * sites, (sites, eig_count))):
        coords[i] = coord
    load_momenta.wait()
    cosine, sine = site_phases(
        lambda i: momenta[0, i], [coords[i] for i in range(3)], extent_x, (sites, eig_count)
    )
    waves[0] = cosine
    waves[1] = sine
    load_slots.wait()
    load_per.wait()
    sink[me] = per[slots[1]].reshape(8, rows, eig_count)

    early = late & (time == 0)

    @pl.when(early)
    def _():
        enter()
        send_sink(jnp.where(line == lines - 1, 0, 1))
        send_near()

    load_eig.wait()
    eig32[...] = eig[...].astype(F32)
    for color in range(3):
        real = eig32[pl.ds(2 * color, sites, stride=6), :]
        imag = eig32[pl.ds(2 * color + 1, sites, stride=6), :]
        wave_real = (waves[0] * real - waves[1] * imag).astype(BF16)
        wave_imag = (waves[1] * real + waves[0] * imag).astype(BF16)
        span = pl.ds(color * sites, sites)
        left[span, :eig_count] = real.astype(BF16)
        left[span, eig_count:] = imag.astype(BF16)
        right[span, :eig_count] = wave_real
        right[span, eig_count:] = wave_imag
    whole = lax.dot_general(
        left[...], right[...], (((0,), (0,)), ((), ())), preferred_element_type=F32
    )
    whole = jnp.concatenate(
        [
            whole[:eig_count, :eig_count] + whole[eig_count:, eig_count:],
            whole[:eig_count, eig_count:] - whole[eig_count:, :eig_count],
        ],
        axis=1,
    )
    part[...] = whole.astype(part.dtype).reshape(hubs, hub_rows, 2 * eig_count)

    def send_red():
        for i in range(hubs):
            j = 2 * (i // 2) + (1 - i % 2) * (1 - 2 * side) + side
            j = jnp.where(me < n // 2, (j + 2) % 4, j)
            copy = remote(
                part.at[j], sums.at[time * n + me], red_recv.at[time], j + n // 4, hub_time
            )
            pl.when((slot != j) | is_leaf)(copy.start)

    def send_turned():
        for k in range(1, n):
            peer = lax.rem(me + k, n)
            remote(turned.at[peer], picked.at[me], turn_recv.at[0], peer).start()

    pl.when(jnp.logical_not(early))(enter)
    send_red()

    @pl.when(jnp.logical_not(early))
    def _():
        send_near()
        pl.when(line == 1)(lambda: send_sink(0))
        pl.when(line == lines - 2)(lambda: send_sink(0))
        pl.when(line == lines - 2)(lambda: send_sink(1))

    load_columns.start()
    load_phases.start()
    first = per[slots[0]].reshape(8 * rows, eig_count).astype(F32)
    turned[...] = first.T.astype(BF16).reshape(n, rows, 8 * rows)
    picked[me] = turned[me]

    @pl.when(line < lines // 2)
    def _():
        pl.when(line == 0)(lambda: send_up(1))
        send_up(2)

    pl.when(is_leaf)(lambda: pl.semaphore_wait(ready.at[0], 1))
    send_turned()
    pl.when((line == 0) | (line == lines - 2))(lambda: send_up(lines - 1))
    pl.when((line == lines - 1) & (time == hub_time))(lambda: send_sink(0))
    pl.when(line == lines - 1)(lambda: send_sink(1))
    pl.when(line == lines - 1)(lambda: send_sink(2))

    def forward(origin):
        owner = 2 * origin + side
        arrived(sink.at[owner], line_recv.at[origin])
        return owner

    def pass_on(origin):
        owner = forward(origin)
        remote(sink.at[owner], sink.at[owner], near_recv.at[0], partner).start()

    inner_line = (line > 0) & (line < lines - 1)

    @pl.when(is_hub)
    def _():
        sums[time * n + me] = part[here]
        for other in range(times):
            own = other == times - 1
            if own:
                pl.when(line == 1)(lambda: pass_on(0))
            arrived(sums.at[pl.ds(0, n - own)], red_recv.at[other])
            total = sums[other * n].astype(F32)
            for k in range(1, n):
                total = total + sums[other * n + k].astype(F32)
            source = mfull.at[here] if own else spread.at[other]
            source[...] = total.astype(BF16)
            for k in range(n - own):
                peer = k + (k >= me).astype(jnp.int32) if own else k
                remote(source, mfull.at[here], all_recv.at[0], peer, other).start()

    relays = inner_line & (late | (time == 0))

    @pl.when(inner_line & jnp.logical_not(relays))
    def _():
        pass_on(line - toward)

    @pl.when(relays)
    def _():
        origin = line - toward
        owner = forward(origin)
        ends = me + 2 * toward
        block = sink.at[owner]
        remote(block, block, line_recv.at[line + toward], ends + 1 - 2 * side).start()
        remote(block, block, line_recv.at[origin], ends).start()
        remote(block, block, near_recv.at[0], partner).start()

    @pl.when(inner_line)
    def _():
        pl.when(late | (time < hub_time))(lambda: pass_on(line + toward))
        pass_on(line - 2 * toward)

    plain_end = (line == 0) & (time == hub_time)

    @pl.when(jnp.logical_not(inner_line))
    def _():
        pass_on(line - toward)
        pl.when(plain_end)(lambda: pass_on(line - 2 * toward))
        pass_on(line - 3 * toward)

    arrived(picked.at[pl.ds(0, n - 1)], turn_recv.at[0])
    group = lax.broadcasted_iota(jnp.int32, (rows, eig_count), 1) // rows
    chunks = [None] * 8
    for k in range(n):
        block = picked[k].astype(F32)
        for c in range(8):
            turn = (k - c) % 8
            moved = pltpu.roll(block, turn * rows, 1) if turn else block
            chunks[c] = moved if chunks[c] is None else jnp.where(group == k, moved, chunks[c])
    sources = jnp.concatenate(chunks[0::2] + chunks[1::2], axis=0).astype(BF16)
    load_columns.wait()
    load_phases.wait()
    for g in range(gammas):
        for spin in range(4):
            phase = phases[spin, g]
            place = spin * 4 + columns[spin, g]
            picks[0, 4 * g + spin] = phase * 16 + place
            picks[1, 4 * g + spin] = lax.rem(phase + 3, 4) * 16 + place

    @pl.when(inner_line | plain_end)
    def _():
        arrived(sink.at[pl.ds(0, lines)], near_recv.at[0])

    @pl.when(jnp.logical_not(inner_line | plain_end))
    def _():
        forward(line - 2 * toward)
        arrived(sink.at[me], line_recv.at[line])
        arrived(sink.at[pl.ds(0, lines - 1)], near_recv.at[0])

    @pl.when(is_hub)
    def _():
        arrived(mfull.at[pl.ds(0, hubs - 1)], all_recv.at[0])

    @pl.when(is_leaf)
    def _():
        arrived(mfull, all_recv.at[0])

    half = 4 * rows
    both = jnp.dot(sources, mfull[...].reshape(eig_count, 2 * eig_count), preferred_element_type=F32)
    cross_real = ((both[:half, :eig_count] + both[half:, eig_count:]) * factor).astype(BF16)
    cross_imag = ((both[:half, eig_count:] - both[half:, :eig_count]) * factor).astype(BF16)
    stacked = jnp.concatenate(
        [
            jnp.concatenate([cross_real, -cross_imag], axis=1),
            jnp.concatenate([cross_imag, cross_real], axis=1),
        ],
        axis=0,
    )
    for pair in range(2):
        table = jnp.concatenate(
            [
                jnp.concatenate(
                    [sink[owner, 4 * pair + 2 * i + c] for c in range(2) for owner in range(n)], axis=0
                )
                for i in range(2)
            ],
            axis=1,
        )
        result = jnp.dot(stacked, table, preferred_element_type=F32)
        for i in range(2):
            for spin in range(4):
                place = spin * 4 + 2 * pair + i
                columns_of = slice(i * eig_count, (i + 1) * eig_count)
                real = result[spin * rows : (spin + 1) * rows, columns_of]
                imag = result[(4 + spin) * rows : (5 + spin) * rows, columns_of]
                for turn, block in enumerate((real, -imag, -real, imag)):
                    blocks[turn * 16 + place] = block
    for g in range(gammas):
        for which in range(2):
            term = blocks[picks[which, 4 * g]]
            for spin in range(1, 4):
                term = term + blocks[picks[which, 4 * g + spin]]
            out_ref[pl.ds(2 * g + which, rows, stride=2 * gammas), :] = term

    unit = 4 * rows
    plain = hubs * unit + 2 * lines * 8 * rows + (n - 1) * rows - 8 * rows
    extra = (times * n - 2) * unit

    block = 8 * rows
    direct = time == hub_time
    changes = (
        (inner_line & (late | jnp.logical_not(direct)) & jnp.logical_not(late & direct), block),
        (late & inner_line & direct, 2 * block),
        (jnp.logical_not(late) & inner_line & direct, -block),
        (plain_end, 0),
        (jnp.logical_not(inner_line | plain_end), -block),
    )
    for hub, spreading in ((is_hub, extra), (is_leaf, 0)):
        for some, change in changes:
            pl.when(hub & some)(
                functools.partial(
                    arrived, volume.at[pl.ds(0, plain + spreading + change)], send_sem.at[0]
                )
            )


def store_kernel(source, target, sem):
    copy = pltpu.make_async_copy(source, target, sem.at[0])
    copy.start()
    copy.wait()


def on_device_kernel(eigvecs, perambulator, momenta, source_slots, gamma_columns, gamma_phases):
    sites, eig_count = eigvecs.shape[1], eigvecs.shape[4]
    n = lax.axis_size("space")
    times = lax.axis_size("tm")
    rows = eig_count // n
    total_sites = sites * n
    gammas = gamma_columns.shape[0]
    stored = perambulator.shape[1]
    body = functools.partial(
        kernel, n, sites, total_sites // (LY * LZ), 1.0 / math.sqrt(12.0 * total_sites)
    )
    dma = pltpu.SemaphoreType.DMA
    hbm = pl.BlockSpec(memory_space=pltpu.HBM)
    out = pl.pallas_call(
        body,
        out_shape=pltpu.VMEM((rows * gammas * 2, eig_count), F32),
        in_specs=[hbm] * 6,
        out_specs=pl.BlockSpec(memory_space=pltpu.VMEM),
        scratch_shapes=[
            pltpu.SMEM(momenta.shape, jnp.int32),
            pltpu.SMEM(source_slots.shape, jnp.int32),
            pltpu.SMEM((4, gammas), jnp.int32),
            pltpu.SMEM((4, gammas), jnp.int32),
            pltpu.SMEM((2, 4 * gammas), jnp.int32),
            pltpu.VMEM((sites * 6, eig_count), BF16),
            pltpu.VMEM((sites * 6, eig_count), F32),
            pltpu.VMEM((3, sites, eig_count), F32),
            pltpu.VMEM((2, sites, eig_count), F32),
            pltpu.VMEM((sites * 3, 2 * eig_count), BF16),
            pltpu.VMEM((sites * 3, 2 * eig_count), BF16),
            pltpu.VMEM((stored, 4, 2, rows, eig_count), BF16),
            pltpu.VMEM((n, 8, rows, eig_count), BF16),
            pltpu.VMEM((n, rows, 8 * rows), BF16),
            pltpu.VMEM((n, rows, 8 * rows), BF16),
            pltpu.VMEM((n // 2, 2 * rows, 2 * eig_count), WIRE),
            pltpu.VMEM((times * n, 2 * rows, 2 * eig_count), WIRE),
            pltpu.VMEM((times - 1, 2 * rows, 2 * eig_count), BF16),
            pltpu.VMEM((n // 2, 2 * rows, 2 * eig_count), BF16),
            pltpu.VMEM((64, rows, eig_count), F32),
            pltpu.VMEM((24 * eig_count, eig_count), BF16),
            pltpu.SemaphoreType.REGULAR((1,)),
            pltpu.SemaphoreType.REGULAR((n // 2 - 1,)),
            dma((4,)),
            dma((1,)),
            dma((2,)),
            dma((1,)),
            dma((1,)),
            dma((1,)),
            dma((n // 2,)),
        ],
        compiler_params=pltpu.CompilerParams(
            collective_id=0, has_side_effects=True, vmem_limit_bytes=VMEM_LIMIT
        ),
    )(
        *(
            pltpu.with_memory_space_constraint(array, pltpu.HBM)
            for array in (
                momenta,
                source_slots,
                gamma_columns.T,
                gamma_phases.T,
                eigvecs.reshape(sites * 6, eig_count),
                perambulator[0],
            )
        )
    )
    done = pl.pallas_call(
        store_kernel,
        out_shape=jax.ShapeDtypeStruct(out.shape, F32),
        in_specs=[pl.BlockSpec(memory_space=pl.ANY)],
        out_specs=hbm,
        scratch_shapes=[dma((1,))],
        compiler_params=pltpu.CompilerParams(vmem_limit_bytes=VMEM_LIMIT),
    )(out)
    return done.reshape(1, rows, 1, gammas, 2, eig_count)


def on_device_plain(eigvecs, perambulator, momenta, source_slots, gamma_columns, gamma_phases):
    sites, eig_count = eigvecs.shape[1], eigvecs.shape[4]
    n = lax.axis_size("space")
    total_sites = sites * n
    extent_x = total_sites // (LY * LZ)
    factor = 1.0 / math.sqrt(12.0 * total_sites)
    first_site = lax.axis_index("space") * sites
    chosen = jnp.take(perambulator[0], source_slots, axis=0)
    sinks = lax.all_gather(chosen[1], "space", axis=2, tiled=True)
    turned = lax.all_to_all(chosen[0], "space", split_axis=3, concat_axis=2, tiled=True)
    real = eigvecs[0, :, :, 0].astype(F32)
    imag = eigvecs[0, :, :, 1].astype(F32)
    flat = eigvecs[0].reshape(sites * 6, eig_count)
    tables = []
    for p in range(momenta.shape[0]):
        cosine, sine = site_phases(
            lambda i, p=p: momenta[p, i], site_coords(first_site, (sites, 1, 1)), extent_x, (sites, 1, 1)
        )
        wave_real = cosine * real - sine * imag
        wave_imag = sine * real + cosine * imag
        upper = jnp.concatenate([wave_real, wave_imag], axis=2)
        lower = jnp.concatenate([wave_imag, -wave_real], axis=2)
        waves = jnp.stack([upper, lower], axis=2).astype(BF16).reshape(sites * 6, 2 * eig_count)
        tables.append(
            lax.dot_general(flat, waves, (((0,), (0,)), ((), ())), preferred_element_type=F32)
        )
    whole = lax.psum(jnp.stack(tables), "space").astype(BF16)
    turned_whole = jnp.concatenate([whole[:, :, eig_count:], -whole[:, :, :eig_count]], axis=2)
    both = jnp.stack([whole, turned_whole], axis=1)
    cross = jnp.einsum("skla,pklm->aspm", turned, both, preferred_element_type=F32)
    cross_real, cross_imag = cross[..., :eig_count], cross[..., eig_count:]
    stacked = jnp.stack(
        [
            jnp.stack([cross_real, -cross_imag], axis=-2),
            jnp.stack([cross_imag, cross_real], axis=-2),
        ],
        axis=3,
    ).astype(BF16)
    blocks = jnp.einsum("asphkl,tklb->apsthb", stacked, sinks, preferred_element_type=F32)
    spins = jnp.arange(4, dtype=jnp.int32)
    matches = (gamma_columns[:, :, None] == spins).astype(F32)
    real_sign = (gamma_phases == 0).astype(F32) - (gamma_phases == 2).astype(F32)
    imag_sign = (gamma_phases == 1).astype(F32) - (gamma_phases == 3).astype(F32)
    mix_real = matches * real_sign[:, :, None]
    mix_imag = matches * imag_sign[:, :, None]
    mix = jnp.stack(
        [jnp.stack([mix_real, -mix_imag], axis=-1), jnp.stack([mix_imag, mix_real], axis=-1)],
        axis=1,
    )
    meson = factor * jnp.einsum("gosth,apsthb->apgob", mix, blocks, precision=lax.Precision.HIGHEST)
    return meson[None]


def on_device(eigvecs, perambulator, momenta, *rest):
    n = lax.axis_size("space")
    rows = perambulator.shape[4]
    small = eigvecs.shape[1] % 16 == 0 and eigvecs.shape[4] == 128
    if rows == 16 and n == 8 and lax.axis_size("tm") == 2 and momenta.shape[0] == 1 and small:
        return on_device_kernel(eigvecs, perambulator, momenta, *rest)
    return on_device_plain(eigvecs, perambulator, momenta, *rest)


def solution(mesh):
    in_specs = (
        P(("cfg", "tm"), "space", None, None, None),
        P(("cfg", "tm"), None, None, None, "space", None),
        P(),
        P(),
        P(),
        P(),
    )
    out_specs = P(("cfg", "tm"), "space", None, None, None, None)
    return jax.shard_map(
        on_device, mesh=mesh, in_specs=in_specs, out_specs=out_specs, check_vma=False
    )
```
